256 devices in a mesh: head: 16 (over y, x), batch: 16 (over z, core).
Axes of the slice: x: 4, y: 4, z: 8, core: 2. Of those that a mesh axis runs over, the one named last changes fastest.
Arguments:
- hidden_in: bfloat16 [16, 256, 4096], P('batch', None, 'head')
- w_query: bfloat16 [4096, 4096], P('batch', 'head'), may hold values from -0.09375 to 0.09375
- w_key: bfloat16 [4096, 4096], P('batch', 'head'), may hold values from -0.09375 to 0.09375
- w_value: bfloat16 [4096, 4096], P('batch', 'head'), may hold values from -0.09375 to 0.09375
- w_beta: bfloat16 [4096, 32], P('batch', 'head'), may hold values from -0.09375 to 0.09375
- w_out: bfloat16 [4096, 4096], P('head', 'batch'), may hold values from -0.125 to 0.125
- mem_pos: int32 [16, 2, 64], P('batch'), may hold values from 0 to 127, as said below
- memory_in: float32 [16, 32, 128, 128], P('batch', 'head'), may hold values from -6 to 6
Outputs:
- hidden_out: bfloat16 [16, 256, 4096], P('batch', None, 'head')
- memory_out: float32 [16, 32, 128, 128], P('batch', 'head')
The draws below stay inside these ranges and needn't reach their ends.
Inputs may be any that keep to these rules, and one draw needn't show every extreme that they name: `mem_pos`: within each sequence and segment the 64 positions are distinct and ascending.
All inputs are finite; a program needn't handle non-finite values.
Results may differ from the reference program's by a relative error of at most 0.005.
Values may be sent and summed in bfloat16 or wider, within the bound.
A program may use at most 64 MiB of HBM per device.

```python
import jax
import jax.numpy as jnp
from jax import lax

D = 4096
HEADS = 32
DH = 128
SEGS = 2
MEM = 64
SEG_LEN = 128
ROWS = 256
BATCH = 16


def draw_hidden_in(key, part):
    columns = jnp.arange(D, dtype=jnp.float32) / D
    rising = 0.6 * jnp.power(3.0, columns)
    values = jax.random.normal(key, (BATCH, ROWS, D), jnp.float32) * rising
    return values.astype(jnp.bfloat16)


def draw_mem_pos(key, part):
    keys = jax.random.split(jax.random.fold_in(key, 7), BATCH * SEGS)
    orders = jax.vmap(lambda single: jax.random.permutation(single, SEG_LEN))(keys)
    chosen = jnp.sort(orders[:, :MEM], axis=-1)
    return chosen.reshape(BATCH, SEGS, MEM).astype(jnp.int32)


def spiked(entries, rng, source, target, parts, factor):
    def block_of(dim):
        return (jnp.arange(entries.shape[dim]) // (entries.shape[dim] // parts)).reshape((-1,) + (1,) * (entries.ndim - 1 - dim))

    near = jax.random.permutation(rng, parts)[block_of(target)]
    second = (block_of(target) + parts // 2) % parts
    return jnp.where((block_of(source) == near) | (block_of(source) == second), factor * entries, entries)


def block_levels(own_key, shape, cuts, least, largest):
    def one(dim, blocks):
        steps = jax.random.uniform(jax.random.fold_in(jax.random.fold_in(own_key, 6), dim), (blocks,), jnp.float32, least / len(cuts), largest / len(cuts))
        return jnp.repeat(jnp.exp(steps), shape[dim] // blocks).reshape((-1,) + (1,) * (len(shape) - dim - 1))

    gain = one(*cuts[0])
    for cut in cuts[1:]:
        gain = gain * one(*cut)
    return gain


def gaussian(key, shape, deviation, bound, cuts=(), kind=jnp.bfloat16):
    level = block_levels(key, shape, cuts, -0.22, 0.18) if cuts else 1.0
    drawn = jax.random.normal(key, shape, jnp.float32) * deviation * level
    return jnp.minimum(jnp.maximum(drawn, -bound), bound).astype(kind)


def bell_draw_with(rng, extent, spread, most, pieces, heavy, held_as=jnp.bfloat16):
    values = spread * jax.random.normal(rng, extent, jnp.float32)
    if pieces:
        values = values * block_levels(rng, extent, pieces, -0.22, 0.18)
    return jnp.clip(spiked(values, jax.random.fold_in(rng, 3), *heavy), -most, most).astype(held_as)


def setup_inputs(seed: int = 0) -> dict:
    key_of = jax.random.split(jax.random.key(seed), 9)
    hidden_in = draw_hidden_in(jax.random.fold_in(key_of[8], 71), 0)
    w_query = gaussian(key_of[1], (D, HEADS * DH), D ** -0.5, 0.09375, ((0, 16), (1, 16)))
    w_key = gaussian(key_of[2], (D, HEADS * DH), D ** -0.5, 0.09375, ((0, 16), (1, 16)))
    w_value = gaussian(key_of[3], (D, HEADS * DH), D ** -0.5, 0.09375, ((0, 16), (1, 16)))
    w_beta = gaussian(key_of[4], (D, HEADS), D ** -0.5, 0.09375, ((0, 16), (1, 16)))
    w_out = bell_draw_with(key_of[5], (HEADS * DH, D), (HEADS * DH) ** -0.5, 0.125, ((0, 16), (1, 16)), (0, 1, 16, 2.0))
    mem_pos = draw_mem_pos(jax.random.fold_in(key_of[8], 71), 0)
    memory_in = gaussian(key_of[7], (BATCH, HEADS, DH, DH), 1.0, 6.0, ((0, 16), (1, 16)), jnp.float32)
    return dict(hidden_in=hidden_in, w_query=w_query, w_key=w_key, w_value=w_value, w_beta=w_beta, w_out=w_out, mem_pos=mem_pos, memory_in=memory_in)


epsilon = 1e-05

def recur(query, keys, values, beta, state):
    highest = lax.Precision.HIGHEST
    readouts = []
    for segment in range(query.shape[1]):
        readouts.append(jnp.einsum('bhij,blhj->blhi', state, query[:, segment], precision=highest).astype(jnp.bfloat16))
        recalled = jnp.einsum('bhij,bmhj->bmhi', state, keys[:, segment], precision=highest)
        change = beta[:, segment][..., None] * (values[:, segment] - recalled)
        state = state + jnp.einsum('bmhi,bmhj->bhij', change, keys[:, segment], precision=highest)
    return (jnp.stack(readouts, axis=1), state)

def reference(hidden_in, w_query, w_key, w_value, w_beta, w_out, mem_pos, memory_in):
    x_float = hidden_in.astype(jnp.float32)
    mean_square = lax.optimization_barrier(jnp.mean(x_float * x_float, axis=2, keepdims=True))
    normed = (x_float * lax.rsqrt(mean_square + epsilon)).astype(jnp.bfloat16)
    token_rows = normed.reshape(BATCH * ROWS, D)
    query = jnp.dot(token_rows, w_query, preferred_element_type=jnp.float32) * DH ** (-0.5)
    query = query.reshape(BATCH, SEGS, SEG_LEN, HEADS, DH)
    offsets = (jnp.arange(SEGS, dtype=jnp.int32) * SEG_LEN)[None, :, None]
    picked = (mem_pos + offsets).reshape(BATCH, SEGS * MEM).astype(jnp.int32)
    memory_rows = jax.vmap(lambda block, where: jnp.take(block, where, axis=0))(normed, picked)
    memory_rows = memory_rows.reshape(BATCH * SEGS * MEM, D)
    keys = jnp.dot(memory_rows, w_key, preferred_element_type=jnp.float32).reshape(BATCH, SEGS, MEM, HEADS, DH)
    keys = keys * lax.rsqrt(lax.optimization_barrier(jnp.sum(keys * keys, axis=-1, keepdims=True)) + 1e-06)
    values = jnp.dot(memory_rows, w_value, preferred_element_type=jnp.float32).reshape(BATCH, SEGS, MEM, HEADS, DH)
    beta = jax.nn.sigmoid(jnp.dot(memory_rows, w_beta, preferred_element_type=jnp.float32)).reshape(BATCH, SEGS, MEM, HEADS)
    readout, state = recur(query, keys, values, beta, memory_in)
    readout = readout.reshape(BATCH * ROWS, HEADS * DH)
    mixed = jnp.dot(readout, w_out, preferred_element_type=jnp.float32)
    hidden_out = (mixed + x_float.reshape(BATCH * ROWS, D)).astype(jnp.bfloat16).reshape(BATCH, ROWS, D)
    return (hidden_out, state)
```

```python
import jax
import jax.numpy as jnp
from jax import lax
from jax.experimental import pallas as pl
from jax.experimental.pallas import tpu as pltpu
from jax.sharding import Mesh
from jax.sharding import PartitionSpec as P

HEAD = ("y", "x")
BATCH = ("z", "c")
EPS = 1e-05
F32 = jnp.float32
BF16 = jnp.bfloat16
HIGHEST = lax.Precision.HIGHEST
NN = (((1,), (0,)), ((), ()))
NT = (((1,), (1,)), ((), ()))
TN = (((0,), (0,)), ((), ()))


def dot(a, b, dims=NN, precision=None):
    return lax.dot_general(a, b, dims, precision=precision, preferred_element_type=F32)


class Copies:
    def __init__(self, send, recv):
        self.send, self.recv, self.count, self.sent = send, recv, 0, []

    def post(self, src, dst, to, recv=None):
        slot = self.count
        self.count += 1
        copy = pltpu.make_async_remote_copy(
            src_ref=src,
            dst_ref=dst,
            send_sem=self.send.at[slot],
            recv_sem=self.recv.at[slot],
            device_id=to,
            device_id_type=pl.DeviceIdType.MESH,
        )
        copy.start()
        self.sent.append(copy)
        return slot

    def arrived(self, slot, ref):
        pltpu.make_async_copy(ref, ref, self.recv.at[slot]).wait()

    def drain(self):
        for copy in self.sent:
            copy.wait_send()


def kernel(
    x_in, wq_in, wk_in, wv_in, wb_in, wo_in, pos_in, mem_in,
    out_ref, memory_ref,
    xg, xn, xm, gv, gq, gk, go, parts, wb_v, pos_v, state,
    acc_q, acc_k, acc_v, logits, readout,
    half_a, half_b, full_a, full_b, sum_a, sum_b, half2_a, half2_b, full2_a, full2_b,
    local, send, recv,
):
    y, x, z, c = (lax.axis_index(n) for n in ("y", "x", "z", "c"))
    ny = lambda d: lax.rem(y + (d % 4), 4)
    nx = lambda d: lax.rem(x + (d % 4), 4)
    nz = lambda d: lax.rem(z + (d % 8), 8)
    up, down = {"z": nz(1)}, {"z": nz(-1)}
    xp, xd = {"x": nx(1)}, {"x": nx(-1)}
    yp, yd = {"y": ny(1)}, {"y": ny(-1)}
    partner = {"c": 1 - c}
    mine = z * 2 + c

    barrier = pltpu.get_barrier_semaphore()
    for peer in (up, down, xp, xd, yp, yd, partner):
        pl.semaphore_signal(barrier, inc=1, device_id=peer, device_id_type=pl.DeviceIdType.MESH)

    loads = [
        (wb_in, wb_v),
        (wv_in, gv.at[mine]),
        (wq_in, gq.at[mine]),
        (x_in.at[0], xg.at[y, x]),
        (wk_in, gk.at[mine, 0:256]),
        (wo_in, go.at[mine]),
        (pos_in.at[0], pos_v),
        (mem_in.at[0], state),
    ]
    fetched = []
    for i, (src, dst) in enumerate(loads):
        copy = pltpu.make_async_copy(src, dst, local.at[i])
        copy.start()
        fetched.append(copy)

    fetched[0].wait()
    rows = jnp.concatenate([wb_v[...].astype(F32), jnp.zeros((14, 256), F32)], axis=0)
    gk[mine, 256:272, :] = rows.astype(BF16)
    for copy in fetched[1:]:
        copy.wait()

    pl.semaphore_wait(barrier, 7)
    net = Copies(send, recv)

    def pass_on(buf, block, to):
        return net.post(buf.at[block], buf.at[block], to)

    main = (gv, gq, gk)
    from_down, from_up, from_partner = {}, {}, {}

    def send_own(buf, m):
        from_down[m] = pass_on(buf, mine, up)
        from_up[m] = pass_on(buf, mine, down)

    def give_partner(buf, d, m):
        block = nz(d) * 2 + c
        from_partner[m, d] = pass_on(buf, block, partner)

    for m, buf in enumerate(main):
        send_own(buf, m)
    for m, buf in enumerate(main):
        give_partner(buf, 0, m)

    a0, a1, b0, b1 = slice(0, 64), slice(64, 128), slice(128, 192), slice(192, 256)
    top, low = slice(0, 128), slice(128, 256)

    def same(ref, to):
        return net.post(ref, ref, to)

    own_a, own_b = xg.at[y, x, top], xg.at[y, x, low]
    s = [same(own_a, xp), same(own_a, xd), same(own_b, yp), same(own_b, yd)]
    net.arrived(s[0], xg.at[y, nx(-1), top])
    f0 = same(xg.at[y, nx(-1), a0], xp)
    net.arrived(s[1], xg.at[y, nx(1), top])
    f1 = same(xg.at[y, nx(1), a1], xd)
    net.arrived(s[2], xg.at[ny(-1), x, low])
    f2 = same(xg.at[ny(-1), x, b0], yp)
    net.arrived(s[3], xg.at[ny(1), x, low])
    f3 = same(xg.at[ny(1), x, b1], yd)
    net.arrived(f0, xg.at[y, nx(2), a0])
    net.arrived(f1, xg.at[y, nx(2), a1])
    rows_a = lambda yy, r: xg.at[yy, :, r]
    s0 = same(rows_a(y, top), yp)
    s1 = same(rows_a(y, top), yd)
    net.arrived(f2, xg.at[ny(2), x, b0])
    net.arrived(f3, xg.at[ny(2), x, b1])
    rows_b = lambda xx, r: xg.at[:, xx, r]
    s2 = same(rows_b(x, low), xp)
    s3 = same(rows_b(x, low), xd)

    def relay(buf, m, d):
        net.arrived(from_down[m], buf.at[nz(-d) * 2 + c])
        ahead = pass_on(buf, nz(-d) * 2 + c, up)
        net.arrived(from_up[m], buf.at[nz(d) * 2 + c])
        behind = pass_on(buf, nz(d) * 2 + c, down)
        give_partner(buf, -d, m)
        give_partner(buf, d, m)
        from_down[m], from_up[m] = ahead, behind

    def relay_half(buf, m):
        lo, hi = nz(-3) * 2 + c, nz(3) * 2 + c
        net.arrived(from_down[m], buf.at[lo])
        part = buf.at[lo, 0:128]
        ahead = net.post(part, part, up)
        net.arrived(from_up[m], buf.at[hi])
        part = buf.at[hi, 128:]
        behind = net.post(part, part, down)
        give_partner(buf, -3, m)
        give_partner(buf, 3, m)
        from_down[m], from_up[m] = ahead, behind

    def far(buf, m):
        block = nz(4) * 2 + c
        net.arrived(from_down[m], buf.at[block, 0:128])
        net.arrived(from_up[m], buf.at[block, 128:])
        give_partner(buf, 4, m)

    def take(buf, m, d):
        net.arrived(from_partner[m, d], buf.at[nz(d) * 2 + (1 - c)])

    for m, buf in enumerate(main):
        relay(buf, m, 1)

    net.arrived(s0, rows_a(ny(-1), top))
    f0 = same(rows_a(ny(-1), a0), yp)
    net.arrived(s1, rows_a(ny(1), top))
    f1 = same(rows_a(ny(1), a1), yd)
    net.arrived(s2, rows_b(nx(-1), low))
    f2 = same(rows_b(nx(-1), b0), xp)
    net.arrived(s3, rows_b(nx(1), low))
    f3 = same(rows_b(nx(1), b1), xd)
    net.arrived(f0, rows_a(ny(2), a0))
    net.arrived(f1, rows_a(ny(2), a1))
    net.arrived(f2, rows_b(nx(2), b0))
    net.arrived(f3, rows_b(nx(2), b1))

    def squares(i, total):
        v = xg[i // 4, lax.rem(i, 4)].astype(F32)
        return total + v * v

    total = lax.fori_loop(0, 16, squares, jnp.zeros((256, 256), F32))
    scale = lax.rsqrt(jnp.sum(total, axis=1, keepdims=True) * (1.0 / 4096) + EPS)
    row = lax.broadcasted_iota(jnp.int32, (256, 128), 0)
    where = jnp.concatenate([pos_v[0:1, :], pos_v[1:2, :] + 128], axis=1)
    chosen = jnp.where(row == where, 1.0, 0.0).T.astype(BF16)

    def normalise(i, carry):
        v = xg[i // 4, lax.rem(i, 4)].astype(F32)
        n = (v * scale).astype(BF16)
        xn[i] = n
        xm[i] = dot(chosen, n).astype(BF16)
        return carry

    lax.fori_loop(0, 16, normalise, 0)

    acc_q[...] = jnp.zeros_like(acc_q)
    acc_k[...] = jnp.zeros_like(acc_k)
    acc_v[...] = jnp.zeros_like(acc_v)
    logits[...] = jnp.zeros_like(logits)

    def project(block):
        rows = xm[block]
        acc_v[...] += dot(rows, gv[block])
        acc_q[...] += dot(xn[block], gq[block])
        acc_k[...] += dot(rows, gk[block, 0:256])
        logits[...] += dot(rows, gk[block, 256:272], NT)

    def project_pair(d):
        for m, buf in enumerate(main):
            take(buf, m, d)
        project(nz(d) * 2)
        project(nz(d) * 2 + 1)

    project_pair(0)
    for m, buf in enumerate(main):
        relay(buf, m, 2)
    send_own(go, 3)
    give_partner(go, 0, 3)
    project_pair(-1)
    project_pair(1)
    for m, buf in enumerate(main):
        relay_half(buf, m)
    project_pair(-2)
    project_pair(2)
    relay(go, 3, 1)
    for m, buf in enumerate(main):
        far(buf, m)
    project_pair(-3)
    project_pair(3)
    relay(go, 3, 2)
    project_pair(4)

    for h in range(2):
        cols = slice(h * 128, h * 128 + 128)
        q = acc_q[:, cols] * (128.0 ** -0.5)
        k = acc_k[:, cols]
        k = k * lax.rsqrt(jnp.sum(k * k, axis=1, keepdims=True) + 1e-06)
        v = acc_v[:, cols]
        beta = jax.nn.sigmoid(logits[:, h:h + 1])
        st = state[h]
        for seg in range(2):
            m = slice(seg * 64, seg * 64 + 64)
            t = slice(seg * 128, seg * 128 + 128)
            readout[t, cols] = dot(q[t], st, NT, HIGHEST).astype(BF16)
            change = beta[m] * (v[m] - dot(k[m], st, NT, HIGHEST))
            st = st + dot(change, k[m], TN, HIGHEST)
        memory_ref[0, h] = st

    relay_half(go, 3)
    far(go, 3)
    for d in (0, -1, 1, -2, 2, -3, 3, 4):
        take(go, 3, d)

    def partial(i, carry):
        parts[i // 4, lax.rem(i, 4)] = dot(readout[...], go[i]).astype(BF16)
        return carry

    lax.fori_loop(0, 16, partial, 0)

    h0 = net.post(parts.at[:, nx(2), a0], half_a.at[0], xp)
    h1 = net.post(parts.at[:, nx(2), a1], half_a.at[1], xd)
    h2 = net.post(parts.at[ny(2), :, b0], half_b.at[0], yp)
    h3 = net.post(parts.at[ny(2), :, b1], half_b.at[1], yd)

    def add(dst, src):
        dst[...] = (dst[...].astype(F32) + src[...].astype(F32)).astype(BF16)

    net.arrived(h0, half_a.at[0])
    add(parts.at[:, nx(1), a0], half_a.at[0])
    h0 = net.post(parts.at[:, nx(1), top], full_a.at[0], xp)
    net.arrived(h1, half_a.at[1])
    add(parts.at[:, nx(-1), a1], half_a.at[1])
    h1 = net.post(parts.at[:, nx(-1), top], full_a.at[1], xd)
    net.arrived(h2, half_b.at[0])
    add(parts.at[ny(1), :, b0], half_b.at[0])
    h2 = net.post(parts.at[ny(1), :, low], full_b.at[0], yp)
    net.arrived(h3, half_b.at[1])
    add(parts.at[ny(-1), :, b1], half_b.at[1])
    h3 = net.post(parts.at[ny(-1), :, low], full_b.at[1], yd)

    net.arrived(h0, full_a.at[0])
    net.arrived(h1, full_a.at[1])
    sum_a[...] = (
        parts[:, x, top].astype(F32) + full_a[0].astype(F32) + full_a[1].astype(F32)
    ).astype(BF16)
    g0 = net.post(sum_a.at[ny(2), a0], half2_a.at[0], yp)
    g1 = net.post(sum_a.at[ny(2), a1], half2_a.at[1], yd)
    net.arrived(h2, full_b.at[0])
    net.arrived(h3, full_b.at[1])
    sum_b[...] = (
        parts[y, :, low].astype(F32) + full_b[0].astype(F32) + full_b[1].astype(F32)
    ).astype(BF16)
    g2 = net.post(sum_b.at[nx(2), a0], half2_b.at[0], xp)
    g3 = net.post(sum_b.at[nx(2), a1], half2_b.at[1], xd)

    net.arrived(g0, half2_a.at[0])
    add(sum_a.at[ny(1), a0], half2_a.at[0])
    g0 = net.post(sum_a.at[ny(1)], full2_a.at[0], yp)
    net.arrived(g1, half2_a.at[1])
    add(sum_a.at[ny(-1), a1], half2_a.at[1])
    g1 = net.post(sum_a.at[ny(-1)], full2_a.at[1], yd)
    net.arrived(g2, half2_b.at[0])
    add(sum_b.at[nx(1), a0], half2_b.at[0])
    g2 = net.post(sum_b.at[nx(1)], full2_b.at[0], xp)
    net.arrived(g3, half2_b.at[1])
    add(sum_b.at[nx(-1), a1], half2_b.at[1])
    g3 = net.post(sum_b.at[nx(-1)], full2_b.at[1], xd)

    net.arrived(g0, full2_a.at[0])
    net.arrived(g1, full2_a.at[1])
    mixed = sum_a[y].astype(F32) + full2_a[0].astype(F32) + full2_a[1].astype(F32)
    out_ref[0, top] = (xg[y, x, top].astype(F32) + mixed).astype(BF16)
    net.arrived(g2, full2_b.at[0])
    net.arrived(g3, full2_b.at[1])
    mixed = sum_b[x].astype(F32) + full2_b[0].astype(F32) + full2_b[1].astype(F32)
    out_ref[0, low] = (xg[y, x, low].astype(F32) + mixed).astype(BF16)
    net.drain()


COPIES = 144


def body(hidden_in, w_query, w_key, w_value, w_beta, w_out, mem_pos, memory_in):
    vmem = pltpu.VMEM
    scratch = [
        vmem((4, 4, 256, 256), BF16),
        vmem((16, 256, 256), BF16),
        vmem((16, 128, 256), BF16),
        vmem((16, 256, 256), BF16),
        vmem((16, 256, 256), BF16),
        vmem((16, 272, 256), BF16),
        vmem((16, 256, 256), BF16),
        vmem((4, 4, 256, 256), BF16),
        vmem((2, 256), BF16),
        vmem((2, 64), jnp.int32),
        vmem((2, 128, 128), F32),
        vmem((256, 256), F32),
        vmem((128, 256), F32),
        vmem((128, 256), F32),
        vmem((128, 16), F32),
        vmem((256, 256), BF16),
        vmem((2, 4, 64, 256), BF16),
        vmem((2, 4, 64, 256), BF16),
        vmem((2, 4, 128, 256), BF16),
        vmem((2, 4, 128, 256), BF16),
        vmem((4, 128, 256), BF16),
        vmem((4, 128, 256), BF16),
        vmem((2, 64, 256), BF16),
        vmem((2, 64, 256), BF16),
        vmem((2, 128, 256), BF16),
        vmem((2, 128, 256), BF16),
        pltpu.SemaphoreType.DMA((8,)),
        pltpu.SemaphoreType.DMA((COPIES,)),
        pltpu.SemaphoreType.DMA((COPIES,)),
    ]
    return pl.pallas_call(
        kernel,
        out_shape=(
            jax.ShapeDtypeStruct(hidden_in.shape, BF16),
            jax.ShapeDtypeStruct(memory_in.shape, F32),
        ),
        in_specs=[pl.BlockSpec(memory_space=pltpu.HBM)] * 8,
        out_specs=[pl.BlockSpec(memory_space=vmem)] * 2,
        scratch_shapes=scratch,
        compiler_params=pltpu.CompilerParams(
            collective_id=0, has_side_effects=True
        ),
    )(hidden_in, w_query, w_key, w_value, w_beta.T, w_out, mem_pos, memory_in)


def solution(mesh):
    split = Mesh(mesh.devices.reshape(4, 4, 8, 2), ("y", "x", "z", "c"))
    return jax.shard_map(
        body,
        mesh=split,
        in_specs=(
            P(BATCH, None, HEAD),
            P(BATCH, HEAD),
            P(BATCH, HEAD),
            P(BATCH, HEAD),
            P(BATCH, HEAD),
            P(HEAD, BATCH),
            P(BATCH, None, None),
            P(BATCH, HEAD, None, None),
        ),
        out_specs=(P(BATCH, None, HEAD), P(BATCH, HEAD, None, None)),
        check_vma=False,
    )
```

```python
import functools

import jax
import jax.numpy as jnp
from jax import lax
from jax.experimental import pallas as pl
from jax.experimental.pallas import tpu as pltpu
from jax.sharding import Mesh
from jax.sharding import PartitionSpec as P

HEAD = ("y", "x")
BATCH = ("z", "c")
EPS = 1e-05
F32 = jnp.float32
BF16 = jnp.bfloat16
HIGHEST = lax.Precision.HIGHEST
NN = (((1,), (0,)), ((), ()))
NT = (((1,), (1,)), ((), ()))
TN = (((0,), (0,)), ((), ()))


def dot(a, b, dims=NN, precision=None):
    return lax.dot_general(a, b, dims, precision=precision, preferred_element_type=F32)


class Copies:
    def __init__(self, send, recv):
        self.send, self.recv, self.count, self.sent = send, recv, 0, []

    def post(self, src, dst, to):
        slot = self.count
        self.count += 1
        copy = pltpu.make_async_remote_copy(
            src_ref=src,
            dst_ref=dst,
            send_sem=self.send.at[slot],
            recv_sem=self.recv.at[slot],
            device_id=to,
            device_id_type=pl.DeviceIdType.MESH,
        )
        copy.start()
        self.sent.append(copy)
        return slot

    def same(self, ref, to):
        return self.post(ref, ref, to)

    def arrived(self, slot, ref):
        pltpu.make_async_copy(ref, ref, self.recv.at[slot]).wait()

    def drain(self):
        for copy in self.sent:
            copy.wait_send()
        self.sent = []


class Scatter:
    a0, a1, b0, b1 = slice(0, 32), slice(32, 64), slice(64, 96), slice(96, 128)
    top, low = slice(0, 64), slice(64, 128)

    def __init__(self, net, refs, place, steps, peers):
        self.net = net
        self.parts, self.half_a, self.full_a, self.sum_a, self.half_b, self.full_b, self.sum_b = refs[:7]
        self.half2_a, self.full2_a, self.half2_b, self.full2_b = refs[7:]
        self.x, self.y = place
        self.nx, self.ny = steps
        self.xp, self.xd, self.yp, self.yd = peers

    def multiply(self, rows, weights, two_hops):
        for dy in range(4):
            for dx in range(4):
                if (dx == 2 or dy == 2) == two_hops:
                    yy, xx = self.ny(dy), self.nx(dx)
                    self.parts[yy, xx] = dot(rows, weights[yy * 4 + xx]).astype(BF16)

    def add(self, dst, src):
        dst[...] = (dst[...].astype(F32) + src[...].astype(F32)).astype(BF16)

    def first(self):
        p, nx, ny, post = self.parts, self.nx, self.ny, self.net.post
        self.h = (
            post(p.at[:, nx(2), self.a0], self.half_a.at[0], self.xp),
            post(p.at[:, nx(2), self.a1], self.half_a.at[1], self.xd),
            post(p.at[ny(2), :, self.b0], self.half_b.at[0], self.yp),
            post(p.at[ny(2), :, self.b1], self.half_b.at[1], self.yd),
        )

    def second(self):
        p, nx, ny, post, arrived = self.parts, self.nx, self.ny, self.net.post, self.net.arrived
        arrived(self.h[0], self.half_a.at[0])
        self.add(p.at[:, nx(1), self.a0], self.half_a.at[0])
        f0 = post(p.at[:, nx(1), self.top], self.full_a.at[0], self.xp)
        arrived(self.h[1], self.half_a.at[1])
        self.add(p.at[:, nx(-1), self.a1], self.half_a.at[1])
        f1 = post(p.at[:, nx(-1), self.top], self.full_a.at[1], self.xd)
        arrived(self.h[2], self.half_b.at[0])
        self.add(p.at[ny(1), :, self.b0], self.half_b.at[0])
        f2 = post(p.at[ny(1), :, self.low], self.full_b.at[0], self.yp)
        arrived(self.h[3], self.half_b.at[1])
        self.add(p.at[ny(-1), :, self.b1], self.half_b.at[1])
        f3 = post(p.at[ny(-1), :, self.low], self.full_b.at[1], self.yd)
        self.f = (f0, f1, f2, f3)

    def third(self):
        nx, ny, post, arrived = self.nx, self.ny, self.net.post, self.net.arrived
        arrived(self.f[0], self.full_a.at[0])
        arrived(self.f[1], self.full_a.at[1])
        own = self.parts[:, self.x, self.top].astype(F32)
        self.sum_a[...] = (own + self.full_a[0].astype(F32) + self.full_a[1].astype(F32)).astype(BF16)
        h0 = post(self.sum_a.at[ny(2), self.a0], self.half2_a.at[0], self.yp)
        h1 = post(self.sum_a.at[ny(2), self.a1], self.half2_a.at[1], self.yd)
        arrived(self.f[2], self.full_b.at[0])
        arrived(self.f[3], self.full_b.at[1])
        own = self.parts[self.y, :, self.low].astype(F32)
        self.sum_b[...] = (own + self.full_b[0].astype(F32) + self.full_b[1].astype(F32)).astype(BF16)
        h2 = post(self.sum_b.at[nx(2), self.a0], self.half2_b.at[0], self.xp)
        h3 = post(self.sum_b.at[nx(2), self.a1], self.half2_b.at[1], self.xd)
        self.h = (h0, h1, h2, h3)

    def fourth(self):
        nx, ny, post, arrived = self.nx, self.ny, self.net.post, self.net.arrived
        arrived(self.h[0], self.half2_a.at[0])
        self.add(self.sum_a.at[ny(1), self.a0], self.half2_a.at[0])
        f0 = post(self.sum_a.at[ny(1)], self.full2_a.at[0], self.yp)
        arrived(self.h[1], self.half2_a.at[1])
        self.add(self.sum_a.at[ny(-1), self.a1], self.half2_a.at[1])
        f1 = post(self.sum_a.at[ny(-1)], self.full2_a.at[1], self.yd)
        arrived(self.h[2], self.half2_b.at[0])
        self.add(self.sum_b.at[nx(1), self.a0], self.half2_b.at[0])
        f2 = post(self.sum_b.at[nx(1)], self.full2_b.at[0], self.xp)
        arrived(self.h[3], self.half2_b.at[1])
        self.add(self.sum_b.at[nx(-1), self.a1], self.half2_b.at[1])
        f3 = post(self.sum_b.at[nx(-1)], self.full2_b.at[1], self.xd)
        self.f = (f0, f1, f2, f3)

    def last(self, residual, out, start):
        arrived = self.net.arrived
        for i, (slots, own, full) in enumerate((
            (self.f[:2], self.sum_a.at[self.y], self.full2_a),
            (self.f[2:], self.sum_b.at[self.x], self.full2_b),
        )):
            arrived(slots[0], full.at[0])
            arrived(slots[1], full.at[1])
            mixed = own[...].astype(F32) + full[0].astype(F32) + full[1].astype(F32)
            rows = slice(start + i * 64, start + i * 64 + 64)
            out[rows] = (residual[rows].astype(F32) + mixed).astype(BF16)


def split(v):
    high = v.astype(BF16)
    return high, (v - high.astype(F32)).astype(BF16)


def kernel(*refs):
    dma = pltpu.SemaphoreType.DMA
    pl.run_scoped(functools.partial(layer, *refs), dma((8,)), dma((COPIES,)), dma((COPIES,)))


def layer(
    x_in, wq_in, wk_in, wv_in, wb_in, wo_in, pos_in, mem_in,
    out_ref, memory_ref,
    xg, xn, xm, gv, gq, gk, go, wb_v, pos_v, state, out_v,
    acc_q, acc_k, acc_v, logits, *rest,
):
    sums, (local, send, recv) = rest[:-3], rest[-3:]
    y, x, z, c = (lax.axis_index(n) for n in ("y", "x", "z", "c"))
    ny = lambda d: lax.rem(y + (d % 4), 4)
    nx = lambda d: lax.rem(x + (d % 4), 4)
    nz = lambda d: lax.rem(z + (d % 8), 8)
    up, down = {"z": nz(1)}, {"z": nz(-1)}
    xp, xd = {"x": nx(1)}, {"x": nx(-1)}
    yp, yd = {"y": ny(1)}, {"y": ny(-1)}
    partner = {"c": 1 - c}
    mine = z * 2 + c

    barrier = pltpu.get_barrier_semaphore()
    for peer in (up, down, xp, xd, yp, yd, partner):
        pl.semaphore_signal(barrier, inc=1, device_id=peer, device_id_type=pl.DeviceIdType.MESH)

    loads = [
        (x_in.at[0], xg.at[y, x]),
        (wq_in, gq.at[mine]),
        (wo_in, go.at[mine]),
        (wb_in, wb_v),
        (wv_in, gv.at[mine]),
        (wk_in, gk.at[mine, 0:256]),
        (pos_in.at[0], pos_v),
        (mem_in.at[0], state),
    ]
    fetched = []
    for i, (src, dst) in enumerate(loads):
        copy = pltpu.make_async_copy(src, dst, local.at[i])
        copy.start()
        fetched.append(copy)
    fetched[0].wait()
    with jax.named_scope("enter"):
        pl.semaphore_wait(barrier, 7)
    net = Copies(send, recv)
    same, arrived = net.same, net.arrived

    a0, a1, b0, b1 = slice(0, 64), slice(64, 128), slice(128, 192), slice(192, 256)
    top, low = slice(0, 128), slice(128, 256)
    own_a, own_b = xg.at[y, x, top], xg.at[y, x, low]
    s = [same(own_a, xp), same(own_a, xd), same(own_b, yp), same(own_b, yd)]

    from_down, from_up, from_partner = {}, {}, {}
    Q, O, V, K = range(4)
    bufs = (gq, go, gv, gk)

    def block(d):
        return nz(d) * 2 + c

    def give(m, *distances):
        for d in distances:
            from_partner[m, d] = same(bufs[m].at[block(d)], partner)

    def send_own(m):
        from_down[m] = same(bufs[m].at[block(0)], up)
        from_up[m] = same(bufs[m].at[block(0)], down)

    def relay(m, d):
        arrived(from_down[m], bufs[m].at[block(-d)])
        from_down[m] = same(bufs[m].at[block(-d)], up)
        arrived(from_up[m], bufs[m].at[block(d)])
        from_up[m] = same(bufs[m].at[block(d)], down)

    def relay_half(m):
        rest = slice(128, bufs[m].shape[1])
        arrived(from_down[m], bufs[m].at[block(-3)])
        from_down[m] = same(bufs[m].at[block(-3), top], up)
        arrived(from_up[m], bufs[m].at[block(3)])
        from_up[m] = same(bufs[m].at[block(3), rest], down)

    def far(m):
        rest = slice(128, bufs[m].shape[1])
        arrived(from_down[m], bufs[m].at[block(4), top])
        arrived(from_up[m], bufs[m].at[block(4), rest])
        give(m, 4)

    def take(m, *distances):
        for d in distances:
            arrived(from_partner[m, d], bufs[m].at[nz(d) * 2 + (1 - c)])

    fetched[1].wait()
    send_own(Q)
    fetched[2].wait()
    send_own(O)
    give(Q, 0)
    give(O, 0)
    for copy in fetched[3:]:
        copy.wait()
    rows = jnp.concatenate([wb_v[...].astype(F32), jnp.zeros((14, 256), F32)], axis=0)
    gk[mine, 256:272, :] = rows.astype(BF16)
    acc_q[...] = jnp.zeros_like(acc_q)
    acc_k[...] = jnp.zeros_like(acc_k)
    acc_v[...] = jnp.zeros_like(acc_v)
    logits[...] = jnp.zeros_like(logits)
    row = lax.broadcasted_iota(jnp.int32, (256, 128), 0)
    where = jnp.concatenate([pos_v[0:1, :], pos_v[1:2, :] + 128], axis=1)
    chosen = jnp.where(row == where, 1.0, 0.0).T.astype(BF16)

    arrived(s[0], xg.at[y, nx(-1), top])
    f0 = same(xg.at[y, nx(-1), a0], xp)
    arrived(s[1], xg.at[y, nx(1), top])
    f1 = same(xg.at[y, nx(1), a1], xd)
    arrived(s[2], xg.at[ny(-1), x, low])
    f2 = same(xg.at[ny(-1), x, b0], yp)
    arrived(s[3], xg.at[ny(1), x, low])
    f3 = same(xg.at[ny(1), x, b1], yd)
    relay(Q, 1)
    arrived(f0, xg.at[y, nx(2), a0])
    arrived(f1, xg.at[y, nx(2), a1])
    rows_a = lambda yy, r: xg.at[yy, :, r]
    s0 = same(rows_a(y, top), yp)
    s1 = same(rows_a(y, top), yd)
    arrived(f2, xg.at[ny(2), x, b0])
    arrived(f3, xg.at[ny(2), x, b1])
    rows_b = lambda xx, r: xg.at[:, xx, r]
    s2 = same(rows_b(x, low), xp)
    s3 = same(rows_b(x, low), xd)
    give(Q, -1, 1)
    relay(O, 1)
    give(O, -1, 1)
    relay(Q, 2)
    give(Q, -2, 2)

    arrived(s0, rows_a(ny(-1), top))
    f0 = same(rows_a(ny(-1), a0), yp)
    arrived(s1, rows_a(ny(1), top))
    f1 = same(rows_a(ny(1), a1), yd)
    arrived(s2, rows_b(nx(-1), low))
    f2 = same(rows_b(nx(-1), b0), xp)
    arrived(s3, rows_b(nx(1), low))
    f3 = same(rows_b(nx(1), b1), xd)
    relay(O, 2)
    send_own(V)
    send_own(K)
    give(O, -2, 2)
    give(V, 0)
    give(K, 0)
    relay_half(Q)
    give(Q, -3, 3)
    arrived(f0, rows_a(ny(2), a0))
    arrived(f1, rows_a(ny(2), a1))
    arrived(f2, rows_b(nx(2), b0))
    arrived(f3, rows_b(nx(2), b1))

    def squares(i, total):
        v = xg[i // 4, lax.rem(i, 4)].astype(F32)
        v = v * v
        return total + (v[:, 0:128] + v[:, 128:256])

    with jax.named_scope("squares"):
        total = lax.fori_loop(0, 16, squares, jnp.zeros((256, 128), F32))
        scale = lax.rsqrt(jnp.sum(total, axis=1, keepdims=True) * (1.0 / 4096) + EPS)
    relay_half(O)
    give(O, -3, 3)

    def normalise(i, carry):
        v = xg[i // 4, lax.rem(i, 4)].astype(F32)
        n = (v * scale).astype(BF16)
        xn[i] = n
        xm[i] = dot(chosen, n).astype(BF16)
        return carry

    with jax.named_scope("normalise"):
        lax.fori_loop(0, 16, normalise, 0)

    def project(m, *distances):
        take(m, *distances)
        acc = {Q: acc_q, V: acc_v, K: acc_k}[m]
        left = xn if m == Q else xm
        for d in distances:
            i = nz(d) * 2
            acc[...] += dot(left[i], bufs[m][i, 0:256]) + dot(left[i + 1], bufs[m][i + 1, 0:256])
            if m == K:
                extra = slice(256, 272)
                logits[...] += dot(left[i], gk[i, extra], NT) + dot(left[i + 1], gk[i + 1, extra], NT)

    relay(V, 1)
    give(V, -1, 1)
    with jax.named_scope("project_q"):
        project(Q, 0, -1, 1, -2, 2, -3, 3)
    relay(K, 1)
    give(K, -1, 1)
    far(Q)
    far(O)
    project(Q, 4)

    def wide_state(h):
        high, lo = split(state[h])
        return jnp.concatenate([high, lo, high], axis=1)

    def through(rows, wide):
        high, lo = split(rows)
        return dot(jnp.concatenate([high, high, lo], axis=1), wide, NT)

    cols = (slice(0, 128), slice(128, 256))
    seg_rows = (slice(0, 128), slice(128, 256))
    seg_mem = (slice(0, 64), slice(64, 128))

    def queries(seg, h):
        return acc_q[seg_rows[seg], cols[h]] * (128.0 ** -0.5)

    wides = [wide_state(h) for h in range(2)]
    readout = jnp.concatenate([through(queries(0, h), wides[h]) for h in range(2)], axis=1).astype(BF16)
    take(O, 0, -1, 1, -2, 2, -3, 3, 4)
    scatter = [
        Scatter(net, [r.at[seg] for r in sums], (x, y), (nx, ny), (xp, xd, yp, yd)) for seg in range(2)
    ]
    with jax.named_scope("multiply0"):
        scatter[0].multiply(readout, go, True)
        scatter[0].first()
        scatter[0].multiply(readout, go, False)
    relay(V, 2)
    give(V, -2, 2)
    project(V, 0, -1, 1)
    scatter[0].second()
    relay(K, 2)
    give(K, -2, 2)
    project(K, 0, -1, 1)
    relay_half(V)
    give(V, -3, 3)
    scatter[0].third()
    relay_half(K)
    give(K, -3, 3)
    project(V, -2, 2)
    project(K, -2, 2)
    far(V)
    scatter[0].fourth()
    project(V, -3, 3)
    far(K)
    project(K, -3, 3)
    project(V, 4)
    project(K, 4)

    keys, values, betas = [], [], []
    for h in range(2):
        k = acc_k[:, cols[h]]
        keys.append(k * lax.rsqrt(jnp.sum(k * k, axis=1, keepdims=True) + 1e-06))
        values.append(acc_v[:, cols[h]])
        betas.append(jax.nn.sigmoid(logits[:, h:h + 1]))

    def update(seg, h, recalled):
        m = seg_mem[seg]
        ch, cl = split(betas[h][m] * (values[h][m] - recalled))
        kh, kl = split(keys[h][m])
        state[h] += dot(jnp.concatenate([ch, ch, cl], axis=0), jnp.concatenate([kh, kl, kh], axis=0), TN)

    with jax.named_scope("recur"):
        for h in range(2):
            update(0, h, through(keys[h][seg_mem[0]], wide_state(h)))
        got = []
        for h in range(2):
            got.append(through(jnp.concatenate([queries(1, h), keys[h][seg_mem[1]]], axis=0), wide_state(h)))
        readout = jnp.concatenate([g[0:128] for g in got], axis=1).astype(BF16)
    with jax.named_scope("multiply1"):
        scatter[1].multiply(readout, go, True)
        scatter[1].first()
        scatter[1].multiply(readout, go, False)

    for h in range(2):
        update(1, h, got[h][128:192])
    stored = []
    for h in range(2):
        copy = pltpu.make_async_copy(state.at[h], memory_ref.at[0, h], local.at[h])
        copy.start()
        stored.append(copy)

    def put_out(seg):
        scatter[seg].last(xg.at[y, x], out_v, seg * 128)
        part = seg_rows[seg]
        copy = pltpu.make_async_copy(out_v.at[part], out_ref.at[0, part], local.at[2 + seg])
        copy.start()
        stored.append(copy)

    put_out(0)
    scatter[1].second()
    scatter[1].third()
    scatter[1].fourth()
    put_out(1)
    with jax.named_scope("drain"):
        net.drain()
    with jax.named_scope("stored"):
        for copy in stored:
            copy.wait()


COPIES = 112


def body(hidden_in, w_query, w_key, w_value, w_beta, w_out, mem_pos, memory_in):
    vmem = pltpu.VMEM
    scratch = [
        vmem((4, 4, 256, 256), BF16),
        vmem((16, 256, 256), BF16),
        vmem((16, 128, 256), BF16),
        vmem((16, 256, 256), BF16),
        vmem((16, 256, 256), BF16),
        vmem((16, 272, 256), BF16),
        vmem((16, 256, 256), BF16),
        vmem((2, 256), BF16),
        vmem((2, 64), jnp.int32),
        vmem((2, 128, 128), F32),
        vmem((256, 256), BF16),
        vmem((256, 256), F32),
        vmem((128, 256), F32),
        vmem((128, 256), F32),
        vmem((128, 16), F32),
        vmem((2, 4, 4, 128, 256), BF16),
        vmem((2, 2, 4, 32, 256), BF16),
        vmem((2, 2, 4, 64, 256), BF16),
        vmem((2, 4, 64, 256), BF16),
        vmem((2, 2, 4, 32, 256), BF16),
        vmem((2, 2, 4, 64, 256), BF16),
        vmem((2, 4, 64, 256), BF16),
        vmem((2, 2, 32, 256), BF16),
        vmem((2, 2, 64, 256), BF16),
        vmem((2, 2, 32, 256), BF16),
        vmem((2, 2, 64, 256), BF16),
    ]
    return pl.pallas_call(
        kernel,
        out_shape=(
            jax.ShapeDtypeStruct(hidden_in.shape, BF16),
            jax.ShapeDtypeStruct(memory_in.shape, F32),
        ),
        in_specs=[pl.BlockSpec(memory_space=pltpu.HBM)] * 8,
        out_specs=[pl.BlockSpec(memory_space=pltpu.HBM)] * 2,
        scratch_shapes=scratch,
        compiler_params=pltpu.CompilerParams(
            collective_id=0, has_side_effects=True
        ),
    )(hidden_in, w_query, w_key, w_value, w_beta.T, w_out, mem_pos, memory_in)


def solution(mesh):
    split = Mesh(mesh.devices.reshape(4, 4, 8, 2), ("y", "x", "z", "c"))
    return jax.shard_map(
        body,
        mesh=split,
        in_specs=(
            P(BATCH, None, HEAD),
            P(BATCH, HEAD),
            P(BATCH, HEAD),
            P(BATCH, HEAD),
            P(BATCH, HEAD),
            P(HEAD, BATCH),
            P(BATCH, None, None),
            P(BATCH, HEAD, None, None),
        ),
        out_specs=(P(BATCH, None, HEAD), P(BATCH, HEAD, None, None)),
        check_vma=False,
    )
```

```python
import functools

import jax
import jax.numpy as jnp
from jax import lax
from jax.experimental import pallas as pl
from jax.experimental.pallas import tpu as pltpu
from jax.sharding import Mesh
from jax.sharding import PartitionSpec as P

HEAD = ("y", "x")
BATCH = ("z", "c")
EPS = 1e-05
F32 = jnp.float32
BF16 = jnp.bfloat16
HIGHEST = lax.Precision.HIGHEST
NN = (((1,), (0,)), ((), ()))
NT = (((1,), (1,)), ((), ()))
TN = (((0,), (0,)), ((), ()))


def dot(a, b, dims=NN, precision=None):
    return lax.dot_general(a, b, dims, precision=precision, preferred_element_type=F32)


class Copies:
    def __init__(self, send, recv):
        self.send, self.recv, self.count, self.sent = send, recv, 0, []

    def post(self, src, dst, to):
        slot = self.count
        self.count += 1
        copy = pltpu.make_async_remote_copy(
            src_ref=src,
            dst_ref=dst,
            send_sem=self.send.at[slot],
            recv_sem=self.recv.at[slot],
            device_id=to,
            device_id_type=pl.DeviceIdType.MESH,
        )
        copy.start()
        self.sent.append(copy)
        return slot

    def same(self, ref, to):
        return self.post(ref, ref, to)

    def arrived(self, slot, ref):
        pltpu.make_async_copy(ref, ref, self.recv.at[slot]).wait()

    def drain(self):
        for copy in self.sent:
            copy.wait_send()
        self.sent = []


class Scatter:
    a0, a1, b0, b1 = slice(0, 32), slice(32, 64), slice(64, 96), slice(96, 128)
    top, low = slice(0, 64), slice(64, 128)

    def __init__(self, net, refs, place, steps, peers):
        self.net = net
        self.parts, self.half_a, self.far_a, self.full_a, self.sum_a, self.end_a = refs[:6]
        self.half_b, self.far_b, self.full_b, self.sum_b, self.end_b = refs[6:]
        self.x, self.y = place
        self.nx, self.ny = steps
        self.xp, self.xd, self.yp, self.yd, self.x2, self.y2 = peers

    def multiply(self, rows, weights, hops):
        for dy in range(4):
            for dx in range(4):
                if max((0, 1, 2, 1)[dx], (0, 1, 2, 1)[dy]) == hops:
                    yy, xx = self.ny(dy), self.nx(dx)
                    self.parts[yy, xx] = dot(rows, weights[yy * 4 + xx]).astype(BF16)

    def start(self, rows, weights):
        p, nx, ny, post = self.parts, self.nx, self.ny, self.net.post
        self.multiply(rows, weights, 2)
        self.h = (
            post(p.at[:, nx(2), self.a0], self.half_a.at[0], self.xp),
            post(p.at[:, nx(2), self.a1], self.half_a.at[1], self.xd),
            post(p.at[ny(2), :, self.b0], self.half_b.at[0], self.yp),
            post(p.at[ny(2), :, self.b1], self.half_b.at[1], self.yd),
        )
        self.multiply(rows, weights, 1)
        self.f = (
            post(p.at[:, nx(1), self.top], self.full_a.at[0], self.xp),
            post(p.at[:, nx(-1), self.top], self.full_a.at[1], self.xd),
            post(p.at[ny(1), :, self.low], self.full_b.at[0], self.yp),
            post(p.at[ny(-1), :, self.low], self.full_b.at[1], self.yd),
        )
        self.multiply(rows, weights, 0)

    def hand_on(self):
        passed = []
        for slot, (half, far, i, to) in zip(self.h, (
            (self.half_a, self.far_a, 0, self.xp),
            (self.half_a, self.far_a, 1, self.xd),
            (self.half_b, self.far_b, 0, self.yp),
            (self.half_b, self.far_b, 1, self.yd),
        )):
            self.net.arrived(slot, half.at[i])
            passed.append(self.net.post(half.at[i], far.at[i], to))
        self.h = passed

    def turn(self):
        arrived, post = self.net.arrived, self.net.post
        self.e = []
        for j, (own, full, far, total, end, step, peers) in enumerate((
            (self.parts.at[:, self.x, self.top], self.full_a, self.far_a, self.sum_a, self.end_a, self.ny,
             (self.yp, self.yd, self.y2)),
            (self.parts.at[self.y, :, self.low], self.full_b, self.far_b, self.sum_b, self.end_b, self.nx,
             (self.xp, self.xd, self.x2)),
        )):
            for i in range(2):
                arrived(self.f[2 * j + i], full.at[i])
            near = own[...].astype(F32) + full[0].astype(F32) + full[1].astype(F32)
            for i in range(2):
                arrived(self.h[2 * j + i], far.at[i])
            total[:, 0:32] = (near[:, 0:32] + far[0].astype(F32)).astype(BF16)
            total[:, 32:64] = (near[:, 32:64] + far[1].astype(F32)).astype(BF16)
            self.e.append([
                post(total.at[step(d)], end.at[i], to)
                for i, (d, to) in reversed(tuple(enumerate(zip((1, -1, 2), peers))))
            ][::-1])

    def last(self, residual, out, start):
        for j, (own, end) in enumerate(((self.sum_a.at[self.y], self.end_a), (self.sum_b.at[self.x], self.end_b))):
            mixed = own[...].astype(F32)
            for i in range(3):
                self.net.arrived(self.e[j][i], end.at[i])
                mixed += end[i].astype(F32)
            rows = slice(start + j * 64, start + j * 64 + 64)
            out[rows] = (residual[rows].astype(F32) + mixed).astype(BF16)


def split(v):
    high = v.astype(BF16)
    return high, (v - high.astype(F32)).astype(BF16)


def kernel(*refs):
    dma = pltpu.SemaphoreType.DMA
    pl.run_scoped(functools.partial(layer, *refs), dma((8,)), dma((COPIES,)), dma((COPIES,)))


def layer(
    x_in, wq_in, wk_in, wv_in, wb_in, wo_in, pos_in, mem_in,
    out_ref, memory_ref,
    xg, xn, xm, gv, gq, gk, go, wb_v, pos_v, state, out_v,
    acc_q, acc_k, acc_v, logits, *rest,
):
    sums, (local, send, recv) = rest[:-3], rest[-3:]
    y, x, z, c = (lax.axis_index(n) for n in ("y", "x", "z", "c"))
    ny = lambda d: lax.rem(y + (d % 4), 4)
    nx = lambda d: lax.rem(x + (d % 4), 4)
    nz = lambda d: lax.rem(z + (d % 8), 8)
    up, down = {"z": nz(1)}, {"z": nz(-1)}
    xp, xd = {"x": nx(1)}, {"x": nx(-1)}
    yp, yd = {"y": ny(1)}, {"y": ny(-1)}
    partner = {"c": 1 - c}
    mine = z * 2 + c

    barrier = pltpu.get_barrier_semaphore()
    x2, y2 = {"x": nx(2)}, {"y": ny(2)}
    for peer in (up, down, xp, xd, yp, yd, x2, y2, partner):
        pl.semaphore_signal(barrier, inc=1, device_id=peer, device_id_type=pl.DeviceIdType.MESH)

    loads = [
        (x_in.at[0], xg.at[y, x]),
        (wq_in, gq.at[mine]),
        (wo_in, go.at[mine]),
        (wb_in, wb_v),
        (wv_in, gv.at[mine]),
        (wk_in, gk.at[mine, 0:256]),
        (pos_in.at[0], pos_v),
        (mem_in.at[0], state),
    ]
    fetched = []
    for i, (src, dst) in enumerate(loads):
        copy = pltpu.make_async_copy(src, dst, local.at[i])
        copy.start()
        fetched.append(copy)
    fetched[0].wait()
    with jax.named_scope("enter"):
        pl.semaphore_wait(barrier, 9)
    net = Copies(send, recv)
    same, arrived = net.same, net.arrived

    a0, a1, b0, b1 = slice(0, 64), slice(64, 128), slice(128, 192), slice(192, 256)
    top, low = slice(0, 128), slice(128, 256)
    own_a, own_b = xg.at[y, x, top], xg.at[y, x, low]
    s = [same(own_a, xp), same(own_a, xd), same(own_b, yp), same(own_b, yd)]

    from_down, from_up, from_partner = {}, {}, {}
    Q, O, V, K = range(4)
    bufs = (gq, go, gv, gk)

    def block(d):
        return nz(d) * 2 + c

    def give(m, *distances):
        for d in distances:
            from_partner[m, d] = same(bufs[m].at[block(d)], partner)

    def send_own(m):
        from_down[m] = same(bufs[m].at[block(0)], up)
        from_up[m] = same(bufs[m].at[block(0)], down)

    def relay(m, d):
        arrived(from_down[m], bufs[m].at[block(-d)])
        from_down[m] = same(bufs[m].at[block(-d)], up)
        arrived(from_up[m], bufs[m].at[block(d)])
        from_up[m] = same(bufs[m].at[block(d)], down)

    def relay_half(m):
        rest = slice(128, bufs[m].shape[1])
        arrived(from_down[m], bufs[m].at[block(-3)])
        from_down[m] = same(bufs[m].at[block(-3), top], up)
        arrived(from_up[m], bufs[m].at[block(3)])
        from_up[m] = same(bufs[m].at[block(3), rest], down)

    def far(m):
        rest = slice(128, bufs[m].shape[1])
        arrived(from_down[m], bufs[m].at[block(4), top])
        arrived(from_up[m], bufs[m].at[block(4), rest])
        give(m, 4)

    def take(m, *distances):
        for d in distances:
            arrived(from_partner[m, d], bufs[m].at[nz(d) * 2 + (1 - c)])

    fetched[1].wait()
    send_own(Q)
    fetched[2].wait()
    send_own(O)
    give(Q, 0)
    give(O, 0)
    for copy in fetched[3:]:
        copy.wait()
    rows = jnp.concatenate([wb_v[...].astype(F32), jnp.zeros((14, 256), F32)], axis=0)
    gk[mine, 256:272, :] = rows.astype(BF16)
    acc_q[...] = jnp.zeros_like(acc_q)
    acc_k[...] = jnp.zeros_like(acc_k)
    acc_v[...] = jnp.zeros_like(acc_v)
    logits[...] = jnp.zeros_like(logits)
    row = lax.broadcasted_iota(jnp.int32, (256, 128), 0)
    where = jnp.concatenate([pos_v[0:1, :], pos_v[1:2, :] + 128], axis=1)
    chosen = jnp.where(row == where, 1.0, 0.0).T.astype(BF16)

    arrived(s[0], xg.at[y, nx(-1), top])
    f0 = same(xg.at[y, nx(-1), a0], xp)
    arrived(s[1], xg.at[y, nx(1), top])
    f1 = same(xg.at[y, nx(1), a1], xd)
    arrived(s[2], xg.at[ny(-1), x, low])
    f2 = same(xg.at[ny(-1), x, b0], yp)
    arrived(s[3], xg.at[ny(1), x, low])
    f3 = same(xg.at[ny(1), x, b1], yd)
    relay(Q, 1)
    arrived(f0, xg.at[y, nx(2), a0])
    arrived(f1, xg.at[y, nx(2), a1])
    rows_a = lambda yy, r: xg.at[yy, :, r]
    s0 = same(rows_a(y, top), yp)
    s1 = same(rows_a(y, top), yd)
    arrived(f2, xg.at[ny(2), x, b0])
    arrived(f3, xg.at[ny(2), x, b1])
    rows_b = lambda xx, r: xg.at[:, xx, r]
    s2 = same(rows_b(x, low), xp)
    s3 = same(rows_b(x, low), xd)
    give(Q, -1, 1)
    relay(O, 1)
    give(O, -1, 1)
    relay(Q, 2)
    give(Q, -2, 2)

    arrived(s0, rows_a(ny(-1), top))
    f0 = same(rows_a(ny(-1), a0), yp)
    arrived(s1, rows_a(ny(1), top))
    f1 = same(rows_a(ny(1), a1), yd)
    arrived(s2, rows_b(nx(-1), low))
    f2 = same(rows_b(nx(-1), b0), xp)
    arrived(s3, rows_b(nx(1), low))
    f3 = same(rows_b(nx(1), b1), xd)
    relay(O, 2)
    send_own(V)
    send_own(K)
    give(O, -2, 2)
    give(V, 0)
    give(K, 0)
    relay_half(Q)
    give(Q, -3, 3)
    arrived(f0, rows_a(ny(2), a0))
    arrived(f1, rows_a(ny(2), a1))
    arrived(f2, rows_b(nx(2), b0))
    arrived(f3, rows_b(nx(2), b1))

    def squares(i, total):
        v = xg[i // 4, lax.rem(i, 4)].astype(F32)
        v = v * v
        return total + (v[:, 0:128] + v[:, 128:256])

    with jax.named_scope("squares"):
        total = lax.fori_loop(0, 16, squares, jnp.zeros((256, 128), F32))
        scale = lax.rsqrt(jnp.sum(total, axis=1, keepdims=True) * (1.0 / 4096) + EPS)
    relay_half(O)
    give(O, -3, 3)

    def normalise(i, carry):
        v = xg[i // 4, lax.rem(i, 4)].astype(F32)
        n = (v * scale).astype(BF16)
        xn[i] = n
        xm[i] = dot(chosen, n).astype(BF16)
        return carry

    with jax.named_scope("normalise"):
        lax.fori_loop(0, 16, normalise, 0)

    def project(m, *distances):
        take(m, *distances)
        acc = {Q: acc_q, V: acc_v, K: acc_k}[m]
        left = xn if m == Q else xm
        for d in distances:
            i = nz(d) * 2
            acc[...] += dot(left[i], bufs[m][i, 0:256]) + dot(left[i + 1], bufs[m][i + 1, 0:256])
            if m == K:
                extra = slice(256, 272)
                logits[...] += dot(left[i], gk[i, extra], NT) + dot(left[i + 1], gk[i + 1, extra], NT)

    relay(V, 1)
    give(V, -1, 1)
    with jax.named_scope("project_q"):
        project(Q, 0, -1, 1, -2, 2, -3, 3)
    relay(K, 1)
    give(K, -1, 1)
    far(Q)
    far(O)
    project(Q, 4)

    def wide_state(h):
        high, lo = split(state[h])
        return jnp.concatenate([high, lo, high], axis=1)

    def through(rows, wide):
        high, lo = split(rows)
        return dot(jnp.concatenate([high, high, lo], axis=1), wide, NT)

    cols = (slice(0, 128), slice(128, 256))
    seg_rows = (slice(0, 128), slice(128, 256))
    seg_mem = (slice(0, 64), slice(64, 128))

    def queries(seg, h):
        return acc_q[seg_rows[seg], cols[h]] * (128.0 ** -0.5)

    wides = [wide_state(h) for h in range(2)]
    readout = jnp.concatenate([through(queries(0, h), wides[h]) for h in range(2)], axis=1).astype(BF16)
    take(O, 0, -1, 1, -2, 2, -3, 3, 4)
    scatter = [
        Scatter(net, [r.at[seg] for r in sums], (x, y), (nx, ny), (xp, xd, yp, yd, x2, y2)) for seg in range(2)
    ]
    with jax.named_scope("multiply0"):
        scatter[0].start(readout, go)
    relay(V, 2)
    give(V, -2, 2)
    project(V, 0, -1, 1)
    scatter[0].hand_on()
    relay(K, 2)
    give(K, -2, 2)
    project(K, 0, -1, 1)
    relay_half(V)
    give(V, -3, 3)
    scatter[0].turn()
    relay_half(K)
    give(K, -3, 3)
    project(V, -2, 2)
    project(K, -2, 2)
    far(V)
    project(V, -3, 3)
    far(K)
    project(K, -3, 3)
    project(V, 4)
    project(K, 4)

    keys, values, betas = [], [], []
    for h in range(2):
        k = acc_k[:, cols[h]]
        keys.append(k * lax.rsqrt(jnp.sum(k * k, axis=1, keepdims=True) + 1e-06))
        values.append(acc_v[:, cols[h]])
        betas.append(jax.nn.sigmoid(logits[:, h:h + 1]))

    def update(seg, h, recalled):
        m = seg_mem[seg]
        ch, cl = split(betas[h][m] * (values[h][m] - recalled))
        kh, kl = split(keys[h][m])
        state[h] += dot(jnp.concatenate([ch, ch, cl], axis=0), jnp.concatenate([kh, kl, kh], axis=0), TN)

    with jax.named_scope("recur"):
        for h in range(2):
            update(0, h, through(keys[h][seg_mem[0]], wide_state(h)))
        got = []
        for h in range(2):
            got.append(through(jnp.concatenate([queries(1, h), keys[h][seg_mem[1]]], axis=0), wide_state(h)))
        readout = jnp.concatenate([g[0:128] for g in got], axis=1).astype(BF16)
    with jax.named_scope("multiply1"):
        scatter[1].start(readout, go)

    for h in range(2):
        update(1, h, got[h][128:192])
    stored = []
    for h in range(2):
        copy = pltpu.make_async_copy(state.at[h], memory_ref.at[0, h], local.at[h])
        copy.start()
        stored.append(copy)

    def put_out(seg):
        scatter[seg].last(xg.at[y, x], out_v, seg * 128)
        part = seg_rows[seg]
        copy = pltpu.make_async_copy(out_v.at[part], out_ref.at[0, part], local.at[2 + seg])
        copy.start()
        stored.append(copy)

    scatter[1].hand_on()
    put_out(0)
    scatter[1].turn()
    put_out(1)
    with jax.named_scope("drain"):
        net.drain()
    with jax.named_scope("stored"):
        for copy in stored:
            copy.wait()


COPIES = 116


def body(hidden_in, w_query, w_key, w_value, w_beta, w_out, mem_pos, memory_in):
    vmem = pltpu.VMEM
    scratch = [
        vmem((4, 4, 256, 256), BF16),
        vmem((16, 256, 256), BF16),
        vmem((16, 128, 256), BF16),
        vmem((16, 256, 256), BF16),
        vmem((16, 256, 256), BF16),
        vmem((16, 272, 256), BF16),
        vmem((16, 256, 256), BF16),
        vmem((2, 256), BF16),
        vmem((2, 64), jnp.int32),
        vmem((2, 128, 128), F32),
        vmem((256, 256), BF16),
        vmem((256, 256), F32),
        vmem((128, 256), F32),
        vmem((128, 256), F32),
        vmem((128, 16), F32),
        vmem((2, 4, 4, 128, 256), BF16),
        vmem((2, 2, 4, 32, 256), BF16),
        vmem((2, 2, 4, 32, 256), BF16),
        vmem((2, 2, 4, 64, 256), BF16),
        vmem((2, 4, 64, 256), BF16),
        vmem((2, 3, 64, 256), BF16),
        vmem((2, 2, 4, 32, 256), BF16),
        vmem((2, 2, 4, 32, 256), BF16),
        vmem((2, 2, 4, 64, 256), BF16),
        vmem((2, 4, 64, 256), BF16),
        vmem((2, 3, 64, 256), BF16),
    ]
    return pl.pallas_call(
        kernel,
        out_shape=(
            jax.ShapeDtypeStruct(hidden_in.shape, BF16),
            jax.ShapeDtypeStruct(memory_in.shape, F32),
        ),
        in_specs=[pl.BlockSpec(memory_space=pltpu.HBM)] * 8,
        out_specs=[pl.BlockSpec(memory_space=pltpu.HBM)] * 2,
        scratch_shapes=scratch,
        compiler_params=pltpu.CompilerParams(
            collective_id=0, has_side_effects=True
        ),
    )(hidden_in, w_query, w_key, w_value, w_beta.T, w_out, mem_pos, memory_in)


def solution(mesh):
    split = Mesh(mesh.devices.reshape(4, 4, 8, 2), ("y", "x", "z", "c"))
    return jax.shard_map(
        body,
        mesh=split,
        in_specs=(
            P(BATCH, None, HEAD),
            P(BATCH, HEAD),
            P(BATCH, HEAD),
            P(BATCH, HEAD),
            P(BATCH, HEAD),
            P(HEAD, BATCH),
            P(BATCH, None, None),
            P(BATCH, HEAD, None, None),
        ),
        out_specs=(P(BATCH, None, HEAD), P(BATCH, HEAD, None, None)),
        check_vma=False,
    )
```

```python
import functools

import jax
import jax.numpy as jnp
from jax import lax
from jax.experimental import pallas as pl
from jax.experimental.pallas import tpu as pltpu
from jax.sharding import Mesh
from jax.sharding import PartitionSpec as P

HEAD = ("y", "x")
BATCH = ("z", "c")
EPS = 1e-05
F32 = jnp.float32
BF16 = jnp.bfloat16
HIGHEST = lax.Precision.HIGHEST
NN = (((1,), (0,)), ((), ()))
NT = (((1,), (1,)), ((), ()))
TN = (((0,), (0,)), ((), ()))


def dot(a, b, dims=NN, precision=None):
    return lax.dot_general(a, b, dims, precision=precision, preferred_element_type=F32)


class Copies:
    def __init__(self, send, recv):
        self.send, self.recv, self.count, self.sent = send, recv, 0, {}

    def post(self, src, dst, to):
        slot = self.count
        self.count += 1
        copy = pltpu.make_async_remote_copy(
            src_ref=src,
            dst_ref=dst,
            send_sem=self.send.at[slot],
            recv_sem=self.recv.at[slot],
            device_id=to,
            device_id_type=pl.DeviceIdType.MESH,
        )
        copy.start()
        self.sent[slot] = copy
        return slot

    def same(self, ref, to):
        return self.post(ref, ref, to)

    def arrived(self, slot, ref):
        pltpu.make_async_copy(ref, ref, self.recv.at[slot]).wait()

    def gone(self, slot):
        self.sent.pop(slot).wait_send()

    def drain(self):
        for slot in tuple(self.sent):
            self.gone(slot)


class Scatter:
    HOPS = (2, 1, 3, 0)

    def __init__(self, net, refs, steps, peers):
        self.net, self.steps = net, steps
        self.sides = tuple(zip((refs[:7], refs[7:]), (peers[:3], peers[3:]), (peers[3:], peers[:3])))

    def multiply(self, rows, weights, hops):
        (pa, *_), (pb, *_) = (side[0] for side in self.sides)
        nx, ny = self.steps
        for dy in range(4):
            for dx in range(4):
                if max((0, 1, 2, 1)[dx], (0, 1, 2, 1)[dy]) == hops:
                    got = dot(rows, weights[ny(dy) * 4 + nx(dx)]).astype(BF16)
                    pa[dx, self.HOPS.index(dy)] = got[0:64]
                    pb[dy, self.HOPS.index(dx)] = got[64:128]

    def start(self, rows, weights):
        self.multiply(rows, weights, 2)
        self.h = []
        for (p, half, *_), to, _ in self.sides:
            for i in range(2):
                self.h.append(self.net.post(p.at[2, :, 32 * i:32 * i + 32], half.at[i], to[i]))
        self.multiply(rows, weights, 1)
        self.multiply(rows, weights, 0)

    def push(self, wait):
        if wait:
            for slot in self.h:
                self.net.gone(slot)
        self.f = []
        for part in (slice(0, 1), slice(1, 4)):
            for (p, _, _, full, *_), to, _ in self.sides:
                for i in range(2):
                    self.f.append(self.net.post(p.at[1 + 2 * i, part], full.at[i, part], to[i]))

    def hand_on(self):
        early, late = [], []
        for j, ((_, half, far, *_), to, _) in enumerate(self.sides):
            for i in range(2):
                self.net.arrived(self.h[2 * j + i], half.at[i])
                early.append(self.net.post(half.at[i, 0:1], far.at[i, 0:1], to[i]))
                late.append(self.net.post(half.at[i, 1:4], far.at[i, 1:4], to[i]))
        self.h = early + late

    def turn(self):
        self.e = [[], []]
        for late, part in enumerate((slice(0, 1), slice(1, 4))):
            for j, ((p, _, far, full, total, own, end), _, peers) in enumerate(self.sides):
                for i in range(2):
                    self.net.arrived(self.f[4 * late + 2 * j + i], full.at[i, part])
                near = p[0, part].astype(F32) + full[0, part].astype(F32) + full[1, part].astype(F32)
                for i in range(2):
                    self.net.arrived(self.h[4 * late + 2 * j + i], far.at[i, part])
                passed = jnp.concatenate([far[0, part].astype(F32), far[1, part].astype(F32)], axis=1)
                near = near + passed
                if late:
                    total[1:3] = near[0:2].astype(BF16)
                    own[...] = near[2]
                    self.e[j].append(self.net.post(total.at[1], end.at[1], peers[0]))
                    self.e[j].append(self.net.post(total.at[2], end.at[2], peers[1]))
                else:
                    total[0:1] = near.astype(BF16)
                    self.e[j].append(self.net.post(total.at[0], end.at[0], peers[2]))

    def last(self, residual, out, start):
        for j, ((*_, own, end), _, _) in enumerate(self.sides):
            mixed = own[...]
            for i in range(3):
                self.net.arrived(self.e[j][i], end.at[i])
                mixed += end[i].astype(F32)
            rows = slice(start + j * 64, start + j * 64 + 64)
            out[rows] = (residual[rows].astype(F32) + mixed).astype(BF16)


def split(v):
    high = v.astype(BF16)
    return high, (v - high.astype(F32)).astype(BF16)


def kernel(*refs):
    dma = pltpu.SemaphoreType.DMA
    pl.run_scoped(functools.partial(layer, *refs), dma((8,)), dma((COPIES,)), dma((COPIES,)))


def layer(
    x_in, wq_in, wk_in, wv_in, wb_in, wo_in, pos_in, mem_in,
    out_ref, memory_ref,
    xg, xn, xm, gv, gq, gk, go, wb_v, pos_v, state, out_v,
    acc_q, acc_k, acc_v, logits, *rest,
):
    sums, (local, send, recv) = rest[:-3], rest[-3:]
    y, x, z, c = (lax.axis_index(n) for n in ("y", "x", "z", "c"))
    ny = lambda d: lax.rem(y + (d % 4), 4)
    nx = lambda d: lax.rem(x + (d % 4), 4)
    nz = lambda d: lax.rem(z + (d % 8), 8)
    up, down = {"z": nz(1)}, {"z": nz(-1)}
    xp, xd = {"x": nx(1)}, {"x": nx(-1)}
    yp, yd = {"y": ny(1)}, {"y": ny(-1)}
    partner = {"c": 1 - c}
    mine = z * 2 + c

    barrier = pltpu.get_barrier_semaphore()
    x2, y2 = {"x": nx(2)}, {"y": ny(2)}
    for peer in (up, down, xp, xd, yp, yd, x2, y2, partner):
        pl.semaphore_signal(barrier, inc=1, device_id=peer, device_id_type=pl.DeviceIdType.MESH)

    loads = [
        (x_in.at[0], xg.at[y, x]),
        (wq_in, gq.at[mine]),
        (wo_in, go.at[mine]),
        (wv_in, gv.at[mine]),
        (wb_in, wb_v),
        (wk_in, gk.at[mine, 0:256]),
        (pos_in.at[0], pos_v),
        (mem_in.at[0], state),
    ]
    fetched = []
    for i, (src, dst) in enumerate(loads):
        copy = pltpu.make_async_copy(src, dst, local.at[i])
        copy.start()
        fetched.append(copy)
    fetched[0].wait()
    with jax.named_scope("enter"):
        pl.semaphore_wait(barrier, 9)
    net = Copies(send, recv)
    same, arrived = net.same, net.arrived

    a0, a1, b0, b1 = slice(0, 64), slice(64, 128), slice(128, 192), slice(192, 256)
    top, low = slice(0, 128), slice(128, 256)
    own_a, own_b = xg.at[y, x, top], xg.at[y, x, low]
    s = [same(own_a, xp), same(own_a, xd), same(own_b, yp), same(own_b, yd)]

    from_down, from_up, from_partner = {}, {}, {}
    Q, O, V, K = range(4)
    bufs = (gq, go, gv, gk)
    order = (
        (Q, 0), (O, 0), (V, 0), (Q, 1), (O, 1), (K, 0), (Q, 2), (O, 2), (V, 1), (Q, 3), (O, 3), (K, 1),
        (V, 2, 0), (V, 2, 1), (K, 2, 0), (K, 2, 1), (V, 3), (K, 3),
    )
    leave = {0: 3, 1: 4, 2: 5, 3: 6, 4: 7, 5: 8, 6: 9, 7: 10, 8: 11, 9: 12, 10: 13, 11: 14, 12: 15, 13: 16, 14: 17}

    def block(d):
        return nz(d) * 2 + c

    def give(m, *distances):
        for d in distances:
            from_partner[m, d] = same(bufs[m].at[block(d)], partner)

    def pieces(m, s, later=None):
        rest = slice(128, bufs[m].shape[1])
        if s < 3 and later is None:
            return slice(None), slice(None)
        return (rest, top) if later else (top, rest)

    def issue(i):
        m, s = order[i][:2]
        ahead, behind = pieces(*order[i])
        from_down[i] = same(bufs[m].at[block(-s), ahead], up)
        from_up[i] = same(bufs[m].at[block(s), behind], down)

    def ring(*indices):
        for i in indices:
            m, s, *later = order[i]
            ahead, behind = pieces(*order[i])
            arrived(from_down[i], bufs[m].at[block(-s - 1), ahead])
            arrived(from_up[i], bufs[m].at[block(s + 1), behind])
            if i in leave:
                issue(leave[i])
            if s == 3:
                give(m, 4)
            elif later != [0]:
                give(m, -s - 1, s + 1)

    def take(m, *distances):
        for d in distances:
            arrived(from_partner[m, d], bufs[m].at[nz(d) * 2 + (1 - c)])

    for i in range(3):
        fetched[1 + i].wait()
        issue(i)
    for copy in fetched[4:]:
        copy.wait()
    rows = jnp.concatenate([wb_v[...].astype(F32), jnp.zeros((14, 256), F32)], axis=0)
    gk[mine, 256:272, :] = rows.astype(BF16)
    for m in (Q, O, V, K):
        give(m, 0)
    acc_q[...] = jnp.zeros_like(acc_q)
    acc_k[...] = jnp.zeros_like(acc_k)
    acc_v[...] = jnp.zeros_like(acc_v)
    logits[...] = jnp.zeros_like(logits)
    row = lax.broadcasted_iota(jnp.int32, (256, 128), 0)
    where = jnp.concatenate([pos_v[0:1, :], pos_v[1:2, :] + 128], axis=1)
    chosen = jnp.where(row == where, 1.0, 0.0).T.astype(BF16)

    arrived(s[0], xg.at[y, nx(-1), top])
    f0 = same(xg.at[y, nx(-1), a0], xp)
    arrived(s[1], xg.at[y, nx(1), top])
    f1 = same(xg.at[y, nx(1), a1], xd)
    arrived(s[2], xg.at[ny(-1), x, low])
    f2 = same(xg.at[ny(-1), x, b0], yp)
    arrived(s[3], xg.at[ny(1), x, low])
    f3 = same(xg.at[ny(1), x, b1], yd)
    arrived(f0, xg.at[y, nx(2), a0])
    arrived(f1, xg.at[y, nx(2), a1])
    rows_a = lambda yy, r: xg.at[yy, :, r]
    s0 = same(rows_a(y, top), yp)
    s1 = same(rows_a(y, top), yd)
    arrived(f2, xg.at[ny(2), x, b0])
    arrived(f3, xg.at[ny(2), x, b1])
    rows_b = lambda xx, r: xg.at[:, xx, r]
    s2 = same(rows_b(x, low), xp)
    s3 = same(rows_b(x, low), xd)
    ring(0, 1, 2)

    arrived(s0, rows_a(ny(-1), top))
    f0 = same(rows_a(ny(-1), a0), yp)
    arrived(s1, rows_a(ny(1), top))
    f1 = same(rows_a(ny(1), a1), yd)
    arrived(s2, rows_b(nx(-1), low))
    f2 = same(rows_b(nx(-1), b0), xp)
    arrived(s3, rows_b(nx(1), low))
    f3 = same(rows_b(nx(1), b1), xd)
    ring(3, 4)
    arrived(f0, rows_a(ny(2), a0))
    arrived(f1, rows_a(ny(2), a1))
    arrived(f2, rows_b(nx(2), b0))
    arrived(f3, rows_b(nx(2), b1))

    def squares(i, total):
        v = xg[i // 4, lax.rem(i, 4)].astype(F32)
        v = v * v
        return total + (v[:, 0:128] + v[:, 128:256])

    with jax.named_scope("squares"):
        total = lax.fori_loop(0, 16, squares, jnp.zeros((256, 128), F32))
        scale = lax.rsqrt(jnp.sum(total, axis=1, keepdims=True) * (1.0 / 4096) + EPS)
    ring(5)

    def normalise(i, carry):
        v = xg[i // 4, lax.rem(i, 4)].astype(F32)
        n = (v * scale).astype(BF16)
        xn[i] = n
        xm[i] = dot(chosen, n).astype(BF16)
        return carry

    with jax.named_scope("normalise"):
        lax.fori_loop(0, 16, normalise, 0)

    def project(m, *distances):
        take(m, *distances)
        acc = {Q: acc_q, V: acc_v, K: acc_k}[m]
        left = xn if m == Q else xm
        for d in distances:
            i = nz(d) * 2
            acc[...] += dot(left[i], bufs[m][i, 0:256]) + dot(left[i + 1], bufs[m][i + 1, 0:256])
            if m == K:
                extra = slice(256, 272)
                logits[...] += dot(left[i], gk[i, extra], NT) + dot(left[i + 1], gk[i + 1, extra], NT)

    ring(6)
    with jax.named_scope("project_q"):
        project(Q, 0, -1, 1, -2, 2)
    ring(7, 8, 9, 10)
    project(Q, -3, 3, 4)

    def wide_state(h):
        high, lo = split(state[h])
        return jnp.concatenate([high, lo, high], axis=1)

    def through(rows, wide):
        high, lo = split(rows)
        return dot(jnp.concatenate([high, high, lo], axis=1), wide, NT)

    cols = (slice(0, 128), slice(128, 256))
    seg_rows = (slice(0, 128), slice(128, 256))
    seg_mem = (slice(0, 64), slice(64, 128))

    def queries(seg, h):
        return acc_q[seg_rows[seg], cols[h]] * (128.0 ** -0.5)

    wides = [wide_state(h) for h in range(2)]
    readout = jnp.concatenate([through(queries(0, h), wides[h]) for h in range(2)], axis=1).astype(BF16)
    take(O, 0, -1, 1, -2, 2, -3, 3, 4)
    scatter = [
        Scatter(net, [r.at[seg] for r in sums], (nx, ny), (xp, xd, x2, yp, yd, y2)) for seg in range(2)
    ]
    with jax.named_scope("multiply0"):
        scatter[0].start(readout, go)
        scatter[0].push(False)
    project(V, 0, -1, 1)
    ring(11, 12)
    scatter[0].hand_on()
    ring(13)
    project(K, 0, -1, 1)
    ring(14)
    project(V, -2, 2)
    ring(15)
    project(K, -2, 2)
    ring(16)
    scatter[0].turn()
    project(V, -3, 3)
    ring(17)
    project(K, -3, 3)
    project(V, 4)
    project(K, 4)

    keys, values, betas = [], [], []
    for h in range(2):
        k = acc_k[:, cols[h]]
        keys.append(k * lax.rsqrt(jnp.sum(k * k, axis=1, keepdims=True) + 1e-06))
        values.append(acc_v[:, cols[h]])
        betas.append(jax.nn.sigmoid(logits[:, h:h + 1]))

    def update(seg, h, recalled):
        m = seg_mem[seg]
        ch, cl = split(betas[h][m] * (values[h][m] - recalled))
        kh, kl = split(keys[h][m])
        state[h] += dot(jnp.concatenate([ch, ch, cl], axis=0), jnp.concatenate([kh, kl, kh], axis=0), TN)

    with jax.named_scope("recur"):
        for h in range(2):
            update(0, h, through(keys[h][seg_mem[0]], wide_state(h)))
        got = []
        for h in range(2):
            got.append(through(jnp.concatenate([queries(1, h), keys[h][seg_mem[1]]], axis=0), wide_state(h)))
        readout = jnp.concatenate([g[0:128] for g in got], axis=1).astype(BF16)
    with jax.named_scope("multiply1"):
        scatter[1].start(readout, go)

    for h in range(2):
        update(1, h, got[h][128:192])
    scatter[1].push(True)
    stored = []
    for h in range(2):
        copy = pltpu.make_async_copy(state.at[h], memory_ref.at[0, h], local.at[h])
        copy.start()
        stored.append(copy)

    def put_out(seg):
        scatter[seg].last(xg.at[y, x], out_v, seg * 128)
        part = seg_rows[seg]
        copy = pltpu.make_async_copy(out_v.at[part], out_ref.at[0, part], local.at[2 + seg])
        copy.start()
        stored.append(copy)

    scatter[1].hand_on()
    put_out(0)
    scatter[1].turn()
    put_out(1)
    with jax.named_scope("drain"):
        net.drain()
    with jax.named_scope("stored"):
        for copy in stored:
            copy.wait()


COPIES = 136


def body(hidden_in, w_query, w_key, w_value, w_beta, w_out, mem_pos, memory_in):
    vmem = pltpu.VMEM
    scratch = [
        vmem((4, 4, 256, 256), BF16),
        vmem((16, 256, 256), BF16),
        vmem((16, 128, 256), BF16),
        vmem((16, 256, 256), BF16),
        vmem((16, 256, 256), BF16),
        vmem((16, 272, 256), BF16),
        vmem((16, 256, 256), BF16),
        vmem((2, 256), BF16),
        vmem((2, 64), jnp.int32),
        vmem((2, 128, 128), F32),
        vmem((256, 256), BF16),
        vmem((256, 256), F32),
        vmem((128, 256), F32),
        vmem((128, 256), F32),
        vmem((128, 16), F32),
        vmem((2, 4, 4, 64, 256), BF16),
        vmem((2, 2, 4, 32, 256), BF16),
        vmem((2, 2, 4, 32, 256), BF16),
        vmem((2, 2, 4, 64, 256), BF16),
        vmem((2, 3, 64, 256), BF16),
        vmem((2, 64, 256), F32),
        vmem((2, 3, 64, 256), BF16),
        vmem((2, 4, 4, 64, 256), BF16),
        vmem((2, 2, 4, 32, 256), BF16),
        vmem((2, 2, 4, 32, 256), BF16),
        vmem((2, 2, 4, 64, 256), BF16),
        vmem((2, 3, 64, 256), BF16),
        vmem((2, 64, 256), F32),
        vmem((2, 3, 64, 256), BF16),
    ]
    return pl.pallas_call(
        kernel,
        out_shape=(
            jax.ShapeDtypeStruct(hidden_in.shape, BF16),
            jax.ShapeDtypeStruct(memory_in.shape, F32),
        ),
        in_specs=[pl.BlockSpec(memory_space=pltpu.HBM)] * 8,
        out_specs=[pl.BlockSpec(memory_space=pltpu.HBM)] * 2,
        scratch_shapes=scratch,
        compiler_params=pltpu.CompilerParams(
            collective_id=0, has_side_effects=True
        ),
    )(hidden_in, w_query, w_key, w_value, w_beta.T, w_out, mem_pos, memory_in)


def solution(mesh):
    split = Mesh(mesh.devices.reshape(4, 4, 8, 2), ("y", "x", "z", "c"))
    return jax.shard_map(
        body,
        mesh=split,
        in_specs=(
            P(BATCH, None, HEAD),
            P(BATCH, HEAD),
            P(BATCH, HEAD),
            P(BATCH, HEAD),
            P(BATCH, HEAD),
            P(HEAD, BATCH),
            P(BATCH, None, None),
            P(BATCH, HEAD, None, None),
        ),
        out_specs=(P(BATCH, None, HEAD), P(BATCH, HEAD, None, None)),
        check_vma=False,
    )
```

```python
import functools

import jax
import jax.numpy as jnp
from jax import lax
from jax.experimental import pallas as pl
from jax.experimental.pallas import tpu as pltpu
from jax.sharding import Mesh
from jax.sharding import PartitionSpec as P

HEAD = ("y", "x")
BATCH = ("z", "c")
EPS = 1e-05
F32 = jnp.float32
BF16 = jnp.bfloat16
HIGHEST = lax.Precision.HIGHEST
NN = (((1,), (0,)), ((), ()))
NT = (((1,), (1,)), ((), ()))
TN = (((0,), (0,)), ((), ()))


def dot(a, b, dims=NN, precision=None):
    return lax.dot_general(a, b, dims, precision=precision, preferred_element_type=F32)


class Copies:
    def __init__(self, send, recv):
        self.send, self.recv, self.count, self.sent = send, recv, 0, {}

    def post(self, src, dst, to):
        slot = self.count
        self.count += 1
        copy = pltpu.make_async_remote_copy(
            src_ref=src,
            dst_ref=dst,
            send_sem=self.send.at[slot],
            recv_sem=self.recv.at[slot],
            device_id=to,
            device_id_type=pl.DeviceIdType.MESH,
        )
        copy.start()
        self.sent[slot] = copy
        return slot

    def same(self, ref, to):
        return self.post(ref, ref, to)

    def arrived(self, slot, ref):
        pltpu.make_async_copy(ref, ref, self.recv.at[slot]).wait()

    def gone(self, slot):
        self.sent.pop(slot).wait_send()

    def drain(self):
        for slot in tuple(self.sent):
            self.gone(slot)


class Scatter:
    HOPS = (2, 1, 3, 0)

    def __init__(self, net, refs, steps, peers):
        self.net, self.steps = net, steps
        self.sides = tuple(zip((refs[:7], refs[7:]), (peers[:3], peers[3:]), (peers[3:], peers[:3])))

    def multiply(self, rows, weights, hops):
        (pa, *_), (pb, *_) = (side[0] for side in self.sides)
        nx, ny = self.steps
        for dy in range(4):
            for dx in range(4):
                if max((0, 1, 2, 1)[dx], (0, 1, 2, 1)[dy]) == hops:
                    got = dot(rows, weights[ny(dy) * 4 + nx(dx)]).astype(BF16)
                    pa[dx, self.HOPS.index(dy)] = got[0:64]
                    pb[dy, self.HOPS.index(dx)] = got[64:128]

    def start(self, rows, weights):
        self.multiply(rows, weights, 2)
        self.h = []
        for (p, half, *_), to, _ in self.sides:
            for i in range(2):
                self.h.append(self.net.post(p.at[2, :, 32 * i:32 * i + 32], half.at[i], to[i]))
        self.multiply(rows, weights, 1)
        self.multiply(rows, weights, 0)

    def push(self, wait):
        if wait:
            for slot in self.h:
                self.net.gone(slot)
        self.f = []
        for part in (slice(0, 1), slice(1, 4)):
            for (p, _, _, full, *_), to, _ in self.sides:
                for i in range(2):
                    self.f.append(self.net.post(p.at[1 + 2 * i, part], full.at[i, part], to[i]))

    def hand_on(self):
        early, late = [], []
        for j, ((_, half, far, *_), to, _) in enumerate(self.sides):
            for i in range(2):
                self.net.arrived(self.h[2 * j + i], half.at[i])
                early.append(self.net.post(half.at[i, 0:1], far.at[i, 0:1], to[i]))
                late.append(self.net.post(half.at[i, 1:4], far.at[i, 1:4], to[i]))
        self.h = early + late

    def turn(self):
        self.e = [[], []]
        for late, part in enumerate((slice(0, 1), slice(1, 4))):
            for j, ((p, _, far, full, total, own, end), _, peers) in enumerate(self.sides):
                for i in range(2):
                    self.net.arrived(self.f[4 * late + 2 * j + i], full.at[i, part])
                near = p[0, part].astype(F32) + full[0, part].astype(F32) + full[1, part].astype(F32)
                for i in range(2):
                    self.net.arrived(self.h[4 * late + 2 * j + i], far.at[i, part])
                passed = jnp.concatenate([far[0, part].astype(F32), far[1, part].astype(F32)], axis=1)
                near = near + passed
                if late:
                    total[1:3] = near[0:2].astype(BF16)
                    own[...] = near[2]
                    self.e[j].append(self.net.post(total.at[1], end.at[1], peers[0]))
                    self.e[j].append(self.net.post(total.at[2], end.at[2], peers[1]))
                else:
                    total[0:1] = near.astype(BF16)
                    self.e[j].append(self.net.post(total.at[0], end.at[0], peers[2]))

    def last(self, residual, out, start):
        for j, ((*_, own, end), _, _) in enumerate(self.sides):
            mixed = own[...]
            for i in range(3):
                self.net.arrived(self.e[j][i], end.at[i])
                mixed += end[i].astype(F32)
            rows = slice(start + j * 64, start + j * 64 + 64)
            out[rows] = (residual[rows].astype(F32) + mixed).astype(BF16)
            yield rows


def split(v):
    high = v.astype(BF16)
    return high, (v - high.astype(F32)).astype(BF16)


def kernel(*refs):
    dma = pltpu.SemaphoreType.DMA
    pl.run_scoped(functools.partial(layer, *refs), dma((8,)), dma((COPIES,)), dma((COPIES,)))


def layer(
    x_in, wq_in, wk_in, wv_in, wb_in, wo_in, pos_in, mem_in,
    out_ref, memory_ref,
    xg, xn, xm, gv, gq, gk, go, gb, pos_v, state, out_v,
    acc_q, acc_k, acc_v, base, logits, *rest,
):
    sums, (local, send, recv) = rest[:-3], rest[-3:]
    y, x, z, c = (lax.axis_index(n) for n in ("y", "x", "z", "c"))
    ny = lambda d: lax.rem(y + (d % 4), 4)
    nx = lambda d: lax.rem(x + (d % 4), 4)
    nz = lambda d: lax.rem(z + (d % 8), 8)
    up, down = {"z": nz(1)}, {"z": nz(-1)}
    xp, xd = {"x": nx(1)}, {"x": nx(-1)}
    yp, yd = {"y": ny(1)}, {"y": ny(-1)}
    partner = {"c": 1 - c}
    mine = z * 2 + c

    barrier = pltpu.get_barrier_semaphore()
    x2, y2 = {"x": nx(2)}, {"y": ny(2)}
    for peer in (up, down, xp, xd, yp, yd, x2, y2, partner):
        pl.semaphore_signal(barrier, inc=1, device_id=peer, device_id_type=pl.DeviceIdType.MESH)

    loads = [
        (x_in.at[0], xg.at[y, x]),
        (wq_in, gq.at[mine]),
        (wo_in, go.at[mine]),
        (wb_in, gb.at[mine]),
        (wk_in, gk.at[mine]),
        (wv_in, gv.at[mine]),
        (pos_in.at[0], pos_v),
        (mem_in.at[0], state),
    ]
    fetched = []
    for i, (src, dst) in enumerate(loads):
        copy = pltpu.make_async_copy(src, dst, local.at[i])
        copy.start()
        fetched.append(copy)
    fetched[0].wait()
    with jax.named_scope("enter"):
        pl.semaphore_wait(barrier, 9)
    net = Copies(send, recv)
    same, arrived = net.same, net.arrived

    a0, a1, b0, b1 = slice(0, 64), slice(64, 128), slice(128, 192), slice(192, 256)
    top, low = slice(0, 128), slice(128, 256)
    own_a, own_b = xg.at[y, x, top], xg.at[y, x, low]
    s = [same(own_a, xp), same(own_a, xd), same(own_b, yp), same(own_b, yd)]

    from_down, from_up, from_partner = {}, {}, {}
    Q, O, V, K, B = range(5)
    bufs = (gq, go, gv, gk, gb)
    order = (
        (Q, 0), (O, 0), (K, 0), (Q, 1), (O, 1), (V, 0), (Q, 2), (O, 2), (K, 1), (Q, 3), (O, 3), (V, 1),
        (K, 2, 0), (K, 2, 1), (V, 2, 0), (V, 2, 1), (K, 3), (V, 3),
    )
    leave = {0: 3, 1: 4, 2: 5, 3: 6, 4: 7, 5: 8, 6: 9, 7: 10, 8: 11, 9: 12, 10: 13, 11: 14, 12: 15, 13: 16, 14: 17}

    def block(d):
        return nz(d) * 2 + c

    def give(m, *distances):
        for d in distances:
            from_partner[m, d] = same(bufs[m].at[block(d)], partner)

    def pieces(m, s, later=None):
        if s < 3 and later is None:
            return slice(None), slice(None)
        return (low, top) if later else (top, low)

    def issue(i):
        m, s = order[i][:2]
        ahead, behind = pieces(*order[i])
        from_down[i] = same(bufs[m].at[block(-s), ahead], up)
        from_up[i] = same(bufs[m].at[block(s), behind], down)
        if m == K and order[i][2:] != (1,):
            from_down[B, s] = same(gb.at[block(-s)], up)
            if s < 3:
                from_up[B, s] = same(gb.at[block(s)], down)

    def ring(*indices):
        for i in indices:
            m, s, *later = order[i]
            ahead, behind = pieces(*order[i])
            arrived(from_down[i], bufs[m].at[block(-s - 1), ahead])
            arrived(from_up[i], bufs[m].at[block(s + 1), behind])
            if m == K and later != [1]:
                arrived(from_down[B, s], gb.at[block(-s - 1)])
                if s < 3:
                    arrived(from_up[B, s], gb.at[block(s + 1)])
            if i in leave:
                issue(leave[i])
            if m == K and later != [1]:
                give(B, *((-s - 1, s + 1) if s < 3 else (4,)))
            if s == 3:
                give(m, 4)
            elif later != [0]:
                give(m, -s - 1, s + 1)

    def take(m, *distances):
        for d in distances:
            arrived(from_partner[m, d], bufs[m].at[nz(d) * 2 + (1 - c)])

    for i, needs in enumerate(((1,), (2,), (3, 4))):
        for j in needs:
            fetched[j].wait()
        issue(i)
    for copy in fetched[5:]:
        copy.wait()
    for m in (Q, O, V, K, B):
        give(m, 0)
    acc_q[...] = jnp.zeros_like(acc_q)
    acc_k[...] = jnp.zeros_like(acc_k)
    acc_v[...] = jnp.zeros_like(acc_v)
    logits[...] = jnp.zeros_like(logits)
    row = lax.broadcasted_iota(jnp.int32, (256, 128), 0)
    where = jnp.concatenate([pos_v[0:1, :], pos_v[1:2, :] + 128], axis=1)
    chosen = jnp.where(row == where, 1.0, 0.0).T.astype(BF16)

    arrived(s[0], xg.at[y, nx(-1), top])
    f0 = same(xg.at[y, nx(-1), a0], xp)
    arrived(s[1], xg.at[y, nx(1), top])
    f1 = same(xg.at[y, nx(1), a1], xd)
    arrived(s[2], xg.at[ny(-1), x, low])
    f2 = same(xg.at[ny(-1), x, b0], yp)
    arrived(s[3], xg.at[ny(1), x, low])
    f3 = same(xg.at[ny(1), x, b1], yd)
    arrived(f0, xg.at[y, nx(2), a0])
    arrived(f1, xg.at[y, nx(2), a1])
    rows_a = lambda yy, r: xg.at[yy, :, r]
    s0 = same(rows_a(y, top), yp)
    s1 = same(rows_a(y, top), yd)
    arrived(f2, xg.at[ny(2), x, b0])
    arrived(f3, xg.at[ny(2), x, b1])
    rows_b = lambda xx, r: xg.at[:, xx, r]
    s2 = same(rows_b(x, low), xp)
    s3 = same(rows_b(x, low), xd)
    ring(0, 1, 2)

    arrived(s0, rows_a(ny(-1), top))
    f0 = same(rows_a(ny(-1), a0), yp)
    arrived(s1, rows_a(ny(1), top))
    f1 = same(rows_a(ny(1), a1), yd)
    arrived(s2, rows_b(nx(-1), low))
    f2 = same(rows_b(nx(-1), b0), xp)
    arrived(s3, rows_b(nx(1), low))
    f3 = same(rows_b(nx(1), b1), xd)
    ring(3, 4)
    arrived(f0, rows_a(ny(2), a0))
    arrived(f1, rows_a(ny(2), a1))
    arrived(f2, rows_b(nx(2), b0))
    arrived(f3, rows_b(nx(2), b1))

    def squares(i, total):
        v = xg[i // 4, lax.rem(i, 4)].astype(F32)
        v = v * v
        return total + (v[:, 0:128] + v[:, 128:256])

    with jax.named_scope("squares"):
        total = lax.fori_loop(0, 16, squares, jnp.zeros((256, 128), F32))
        scale = lax.rsqrt(jnp.sum(total, axis=1, keepdims=True) * (1.0 / 4096) + EPS)
    ring(5)

    def normalise(i, carry):
        v = xg[i // 4, lax.rem(i, 4)].astype(F32)
        n = (v * scale).astype(BF16)
        xn[i] = n
        xm[i] = dot(chosen, n).astype(BF16)
        return carry

    with jax.named_scope("normalise"):
        lax.fori_loop(0, 16, normalise, 0)

    def project(m, *distances):
        take(m, *distances)
        if m == K:
            take(B, *distances)
        acc = {Q: acc_q, V: acc_v, K: acc_k}[m]
        left = xn if m == Q else xm
        for d in distances:
            i = nz(d) * 2
            acc[...] += dot(left[i], bufs[m][i]) + dot(left[i + 1], bufs[m][i + 1])
            if m == K:
                logits[...] += dot(left[i], gb[i], NT) + dot(left[i + 1], gb[i + 1], NT)

    ring(6)
    with jax.named_scope("project_q"):
        project(Q, 0, -1, 1, -2, 2)
    ring(7, 8, 9, 10)
    project(Q, -3, 3, 4)

    def wide_state(h):
        high, lo = split(state[h])
        return jnp.concatenate([high, lo, high], axis=1)

    def through(rows, wide):
        high, lo = split(rows)
        return dot(jnp.concatenate([high, high, lo], axis=1), wide, NT)

    cols = (slice(0, 128), slice(128, 256))
    seg_rows = (slice(0, 128), slice(128, 256))
    seg_mem = (slice(0, 64), slice(64, 128))

    def queries(seg, h):
        return acc_q[seg_rows[seg], cols[h]] * (128.0 ** -0.5)

    wides = [wide_state(h) for h in range(2)]
    for h in range(2):
        base[:, cols[h]] = through(queries(1, h), wides[h])
    readout = jnp.concatenate([through(queries(0, h), wides[h]) for h in range(2)], axis=1).astype(BF16)
    take(O, 0, -1, 1, -2, 2, -3, 3, 4)
    scatter = [
        Scatter(net, [r.at[seg] for r in sums], (nx, ny), (xp, xd, x2, yp, yd, y2)) for seg in range(2)
    ]
    with jax.named_scope("multiply0"):
        scatter[0].start(readout, go)
        scatter[0].push(False)
    project(K, 0, -1, 1)
    ring(11, 12)
    scatter[0].hand_on()
    ring(13)
    project(V, 0, -1, 1)
    ring(14)
    project(K, -2, 2)
    ring(15)
    project(V, -2, 2)
    ring(16)
    project(K, -3, 3)
    scatter[0].turn()
    project(V, -3, 3)
    project(K, 4)

    keys, betas, recalls, matches = [], [], [], []
    with jax.named_scope("prepare"):
        for h in range(2):
            k = acc_k[:, cols[h]]
            k = k * lax.rsqrt(jnp.sum(k * k, axis=1, keepdims=True) + 1e-06)
            keys.append(k)
            betas.append(jax.nn.sigmoid(logits[:, h:h + 1]))
            kh, kl = split(k[seg_mem[0]])
            match_high, match_low = split(through(queries(1, h), jnp.concatenate([kh, kl, kh], axis=1)))
            matches.append(jnp.concatenate([match_high, match_high, match_low], axis=1))
            recalls.append(through(k[seg_mem[0]], wide_state(h)))
    ring(17)
    project(V, 4)
    values = [acc_v[:, cols[h]] for h in range(2)]

    def change(seg, h, recalled):
        m = seg_mem[seg]
        return split(betas[h][m] * (values[h][m] - recalled))

    def update(seg, h, changed):
        ch, cl = changed
        kh, kl = split(keys[h][seg_mem[seg]])
        state[h] += dot(jnp.concatenate([ch, ch, cl], axis=0), jnp.concatenate([kh, kl, kh], axis=0), TN)

    with jax.named_scope("recur"):
        changes, readouts = [], []
        for h in range(2):
            ch, cl = change(0, h, recalls[h])
            changes.append((ch, cl))
            readouts.append(base[:, cols[h]] + dot(matches[h], jnp.concatenate([ch, cl, ch], axis=0)))
        readout = jnp.concatenate(readouts, axis=1).astype(BF16)
    with jax.named_scope("multiply1"):
        scatter[1].start(readout, go)

    for h in range(2):
        update(0, h, changes[h])
        update(1, h, change(1, h, through(keys[h][seg_mem[1]], wide_state(h))))
    scatter[1].push(True)
    stored = []
    for h in range(2):
        copy = pltpu.make_async_copy(state.at[h], memory_ref.at[0, h], local.at[h])
        copy.start()
        stored.append(copy)

    def put_out(seg):
        for part in scatter[seg].last(xg.at[y, x], out_v, seg * 128):
            copy = pltpu.make_async_copy(out_v.at[part], out_ref.at[0, part], local.at[len(stored)])
            copy.start()
            stored.append(copy)

    scatter[1].hand_on()
    put_out(0)
    scatter[1].turn()
    with jax.named_scope("drain"):
        net.drain()
    put_out(1)
    with jax.named_scope("stored"):
        for copy in stored:
            copy.wait()


COPIES = 151


def body(hidden_in, w_query, w_key, w_value, w_beta, w_out, mem_pos, memory_in):
    vmem = pltpu.VMEM
    scratch = [
        vmem((4, 4, 256, 256), BF16),
        vmem((16, 256, 256), BF16),
        vmem((16, 128, 256), BF16),
        vmem((16, 256, 256), BF16),
        vmem((16, 256, 256), BF16),
        vmem((16, 256, 256), BF16),
        vmem((16, 256, 256), BF16),
        vmem((16, 2, 256), BF16),
        vmem((2, 64), jnp.int32),
        vmem((2, 128, 128), F32),
        vmem((256, 256), BF16),
        vmem((256, 256), F32),
        vmem((128, 256), F32),
        vmem((128, 256), F32),
        vmem((128, 256), F32),
        vmem((128, 2), F32),
        vmem((2, 4, 4, 64, 256), BF16),
        vmem((2, 2, 4, 32, 256), BF16),
        vmem((2, 2, 4, 32, 256), BF16),
        vmem((2, 2, 4, 64, 256), BF16),
        vmem((2, 3, 64, 256), BF16),
        vmem((2, 64, 256), F32),
        vmem((2, 3, 64, 256), BF16),
        vmem((2, 4, 4, 64, 256), BF16),
        vmem((2, 2, 4, 32, 256), BF16),
        vmem((2, 2, 4, 32, 256), BF16),
        vmem((2, 2, 4, 64, 256), BF16),
        vmem((2, 3, 64, 256), BF16),
        vmem((2, 64, 256), F32),
        vmem((2, 3, 64, 256), BF16),
    ]
    return pl.pallas_call(
        kernel,
        out_shape=(
            jax.ShapeDtypeStruct(hidden_in.shape, BF16),
            jax.ShapeDtypeStruct(memory_in.shape, F32),
        ),
        in_specs=[pl.BlockSpec(memory_space=pltpu.HBM)] * 8,
        out_specs=[pl.BlockSpec(memory_space=pltpu.HBM)] * 2,
        scratch_shapes=scratch,
        compiler_params=pltpu.CompilerParams(
            collective_id=0, has_side_effects=True
        ),
    )(hidden_in, w_query, w_key, w_value, w_beta.T, w_out, mem_pos, memory_in)


def solution(mesh):
    split = Mesh(mesh.devices.reshape(4, 4, 8, 2), ("y", "x", "z", "c"))
    return jax.shard_map(
        body,
        mesh=split,
        in_specs=(
            P(BATCH, None, HEAD),
            P(BATCH, HEAD),
            P(BATCH, HEAD),
            P(BATCH, HEAD),
            P(BATCH, HEAD),
            P(HEAD, BATCH),
            P(BATCH, None, None),
            P(BATCH, HEAD, None, None),
        ),
        out_specs=(P(BATCH, None, HEAD), P(BATCH, HEAD, None, None)),
        check_vma=False,
    )
```

```python
import functools

import jax
import jax.numpy as jnp
from jax import lax
from jax.experimental import pallas as pl
from jax.experimental.pallas import tpu as pltpu
from jax.sharding import Mesh
from jax.sharding import PartitionSpec as P

HEAD = ("y", "x")
BATCH = ("z", "c")
EPS = 1e-05
F32 = jnp.float32
BF16 = jnp.bfloat16
HIGHEST = lax.Precision.HIGHEST
NN = (((1,), (0,)), ((), ()))
NT = (((1,), (1,)), ((), ()))
TN = (((0,), (0,)), ((), ()))


def dot(a, b, dims=NN, precision=None):
    return lax.dot_general(a, b, dims, precision=precision, preferred_element_type=F32)


class Copies:
    def __init__(self, send, recv):
        self.send, self.recv, self.count, self.sent = send, recv, 0, {}

    def post(self, src, dst, to):
        slot = self.count
        self.count += 1
        copy = pltpu.make_async_remote_copy(
            src_ref=src,
            dst_ref=dst,
            send_sem=self.send.at[slot],
            recv_sem=self.recv.at[slot],
            device_id=to,
            device_id_type=pl.DeviceIdType.MESH,
        )
        copy.start()
        self.sent[slot] = copy
        return slot

    def same(self, ref, to):
        return self.post(ref, ref, to)

    def arrived(self, slot, ref):
        pltpu.make_async_copy(ref, ref, self.recv.at[slot]).wait()

    def gone(self, slot):
        self.sent.pop(slot).wait_send()

    def drain(self):
        for slot in tuple(self.sent):
            self.gone(slot)


class Scatter:
    HOPS = (2, 1, 3, 0)

    def __init__(self, net, refs, steps, peers):
        self.net, self.steps = net, steps
        self.sides = tuple(zip((refs[:7], refs[7:]), (peers[:3], peers[3:]), (peers[3:], peers[:3])))

    def multiply(self, rows, weights, hops):
        (pa, *_), (pb, *_) = (side[0] for side in self.sides)
        nx, ny = self.steps
        for dy in range(4):
            for dx in range(4):
                if max((0, 1, 2, 1)[dx], (0, 1, 2, 1)[dy]) == hops:
                    got = dot(rows, weights[ny(dy) * 4 + nx(dx)]).astype(BF16)
                    pa[dx, self.HOPS.index(dy)] = got[0:64]
                    pb[dy, self.HOPS.index(dx)] = got[64:128]

    def start(self, rows, weights):
        self.multiply(rows, weights, 2)
        self.h = []
        for (p, half, *_), to, _ in self.sides:
            for i in range(2):
                self.h.append(self.net.post(p.at[2, :, 32 * i:32 * i + 32], half.at[i], to[i]))
        self.multiply(rows, weights, 1)
        self.multiply(rows, weights, 0)

    def push(self, wait):
        if wait:
            for slot in self.h:
                self.net.gone(slot)
        self.f = []
        for part in (slice(0, 1), slice(1, 4)):
            for (p, _, _, full, *_), to, _ in self.sides:
                for i in range(2):
                    self.f.append(self.net.post(p.at[1 + 2 * i, part], full.at[i, part], to[i]))

    def hand_on(self):
        early, late = [], []
        for j, ((_, half, far, *_), to, _) in enumerate(self.sides):
            for i in range(2):
                self.net.arrived(self.h[2 * j + i], half.at[i])
                early.append(self.net.post(half.at[i, 0:1], far.at[i, 0:1], to[i]))
                late.append(self.net.post(half.at[i, 1:4], far.at[i, 1:4], to[i]))
        self.h = early + late

    def turn(self):
        self.e = [[], []]
        for late, part in enumerate((slice(0, 1), slice(1, 4))):
            for j, ((p, _, far, full, total, own, end), _, peers) in enumerate(self.sides):
                for i in range(2):
                    self.net.arrived(self.f[4 * late + 2 * j + i], full.at[i, part])
                near = p[0, part].astype(F32) + full[0, part].astype(F32) + full[1, part].astype(F32)
                for i in range(2):
                    self.net.arrived(self.h[4 * late + 2 * j + i], far.at[i, part])
                passed = jnp.concatenate([far[0, part].astype(F32), far[1, part].astype(F32)], axis=1)
                near = near + passed
                if late:
                    total[1:3] = near[0:2].astype(BF16)
                    own[...] = near[2]
                    self.e[j].append(self.net.post(total.at[1], end.at[1], peers[0]))
                    self.e[j].append(self.net.post(total.at[2], end.at[2], peers[1]))
                else:
                    total[0:1] = near.astype(BF16)
                    self.e[j].append(self.net.post(total.at[0], end.at[0], peers[2]))

    def last(self, residual, out, start):
        for j, ((*_, own, end), _, _) in enumerate(self.sides):
            mixed = own[...]
            for i in range(3):
                self.net.arrived(self.e[j][i], end.at[i])
                mixed += end[i].astype(F32)
            rows = slice(start + j * 64, start + j * 64 + 64)
            out[rows] = (residual[rows].astype(F32) + mixed).astype(BF16)
            yield rows


def split(v):
    high = v.astype(BF16)
    return high, (v - high.astype(F32)).astype(BF16)


def kernel(*refs):
    dma = pltpu.SemaphoreType.DMA
    pl.run_scoped(functools.partial(layer, *refs), dma((8,)), dma((COPIES,)), dma((COPIES,)))


def layer(
    x_in, wq_in, wk_in, wv_in, wb_in, wo_in, pos_in, mem_in,
    out_ref, memory_ref,
    xg, xn, xm, gv, gq, gk, go, gb, pos_v, state, out_v,
    acc_q, acc_k, acc_v, base, logits, *rest,
):
    sums, (local, send, recv) = rest[:-3], rest[-3:]
    y, x, z, c = (lax.axis_index(n) for n in ("y", "x", "z", "c"))
    ny = lambda d: lax.rem(y + (d % 4), 4)
    nx = lambda d: lax.rem(x + (d % 4), 4)
    nz = lambda d: lax.rem(z + (d % 8), 8)
    up, down = {"z": nz(1)}, {"z": nz(-1)}
    xp, xd = {"x": nx(1)}, {"x": nx(-1)}
    yp, yd = {"y": ny(1)}, {"y": ny(-1)}
    partner = {"c": 1 - c}
    mine = z * 2 + c

    barrier = pltpu.get_barrier_semaphore()
    x2, y2 = {"x": nx(2)}, {"y": ny(2)}
    for peer in (up, down, xp, xd, yp, yd, x2, y2, partner):
        pl.semaphore_signal(barrier, inc=1, device_id=peer, device_id_type=pl.DeviceIdType.MESH)

    loads = [
        (x_in.at[0], xg.at[y, x]),
        (wq_in, gq.at[mine]),
        (wo_in, go.at[mine]),
        (wb_in, gb.at[mine]),
        (wk_in, gk.at[mine]),
        (wv_in, gv.at[mine]),
        (pos_in.at[0], pos_v),
        (mem_in.at[0], state),
    ]
    fetched = []
    for i, (src, dst) in enumerate(loads):
        copy = pltpu.make_async_copy(src, dst, local.at[i])
        copy.start()
        fetched.append(copy)
    fetched[0].wait()
    with jax.named_scope("enter"):
        pl.semaphore_wait(barrier, 9)
    net = Copies(send, recv)
    same, arrived = net.same, net.arrived

    a0, a1, b0, b1 = slice(0, 64), slice(64, 128), slice(128, 192), slice(192, 256)
    top, low = slice(0, 128), slice(128, 256)
    own_a, own_b = xg.at[y, x, top], xg.at[y, x, low]
    s = [same(own_a, xp), same(own_a, xd), same(own_b, yp), same(own_b, yd)]

    from_down, from_up, from_partner = {}, {}, {}
    Q, O, V, K, B = range(5)
    bufs = (gq, go, gv, gk, gb)
    order = (
        (Q, 0), (O, 0), (K, 0), (Q, 1), (O, 1), (V, 0), (Q, 2), (O, 2), (K, 1), (Q, 3), (O, 3), (V, 1),
        (K, 2, 0), (K, 2, 1), (V, 2, 0), (V, 2, 1), (K, 3), (V, 3),
    )
    leave = {0: 3, 1: 4, 2: 5, 3: 6, 4: 7, 5: 8, 6: 9, 7: 10, 8: 11, 9: 12, 10: 13, 11: 14, 12: 15, 13: 16, 14: 17}

    def block(d):
        return nz(d) * 2 + c

    def give(m, *distances):
        for d in distances:
            from_partner[m, d] = same(bufs[m].at[block(d)], partner)

    def pieces(m, s, later=None):
        if s < 3 and later is None:
            return slice(None), slice(None)
        return (low, top) if later else (top, low)

    def issue(i):
        m, s = order[i][:2]
        ahead, behind = pieces(*order[i])
        from_down[i] = same(bufs[m].at[block(-s), ahead], up)
        from_up[i] = same(bufs[m].at[block(s), behind], down)
        if m == K and order[i][2:] != (1,):
            from_down[B, s] = same(gb.at[block(-s)], up)
            if s < 3:
                from_up[B, s] = same(gb.at[block(s)], down)

    def ring(*indices):
        for i in indices:
            m, s, *later = order[i]
            ahead, behind = pieces(*order[i])
            arrived(from_down[i], bufs[m].at[block(-s - 1), ahead])
            arrived(from_up[i], bufs[m].at[block(s + 1), behind])
            if m == K and later != [1]:
                arrived(from_down[B, s], gb.at[block(-s - 1)])
                if s < 3:
                    arrived(from_up[B, s], gb.at[block(s + 1)])
            if i in leave:
                issue(leave[i])
            if m == K and later != [1]:
                give(B, *((-s - 1, s + 1) if s < 3 else (4,)))
            if s == 3:
                give(m, 4)
            elif later != [0]:
                give(m, -s - 1, s + 1)

    def take(m, *distances):
        for d in distances:
            arrived(from_partner[m, d], bufs[m].at[nz(d) * 2 + (1 - c)])

    for i, needs in enumerate(((1,), (2,), (3, 4))):
        for j in needs:
            fetched[j].wait()
        issue(i)
    for copy in fetched[5:]:
        copy.wait()
    for m in (Q, O, V, K, B):
        give(m, 0)
    acc_q[...] = jnp.zeros_like(acc_q)
    acc_k[...] = jnp.zeros_like(acc_k)
    acc_v[...] = jnp.zeros_like(acc_v)
    logits[...] = jnp.zeros_like(logits)
    row = lax.broadcasted_iota(jnp.int32, (256, 128), 0)
    where = jnp.concatenate([pos_v[0:1, :], pos_v[1:2, :] + 128], axis=1)
    chosen = jnp.where(row == where, 1.0, 0.0).T.astype(BF16)

    arrived(s[0], xg.at[y, nx(-1), top])
    f0 = same(xg.at[y, nx(-1), a0], xp)
    arrived(s[1], xg.at[y, nx(1), top])
    f1 = same(xg.at[y, nx(1), a1], xd)
    arrived(s[2], xg.at[ny(-1), x, low])
    f2 = same(xg.at[ny(-1), x, b0], yp)
    arrived(s[3], xg.at[ny(1), x, low])
    f3 = same(xg.at[ny(1), x, b1], yd)
    arrived(f0, xg.at[y, nx(2), a0])
    arrived(f1, xg.at[y, nx(2), a1])
    rows_a = lambda yy, r: xg.at[yy, :, r]
    s0 = same(rows_a(y, top), yp)
    s1 = same(rows_a(y, top), yd)
    arrived(f2, xg.at[ny(2), x, b0])
    arrived(f3, xg.at[ny(2), x, b1])
    rows_b = lambda xx, r: xg.at[:, xx, r]
    s2 = same(rows_b(x, low), xp)
    s3 = same(rows_b(x, low), xd)
    ring(0, 1, 2)

    arrived(s0, rows_a(ny(-1), top))
    f0 = same(rows_a(ny(-1), a0), yp)
    arrived(s1, rows_a(ny(1), top))
    f1 = same(rows_a(ny(1), a1), yd)
    arrived(s2, rows_b(nx(-1), low))
    f2 = same(rows_b(nx(-1), b0), xp)
    arrived(s3, rows_b(nx(1), low))
    f3 = same(rows_b(nx(1), b1), xd)
    ring(3, 4)
    arrived(f0, rows_a(ny(2), a0))
    arrived(f1, rows_a(ny(2), a1))
    arrived(f2, rows_b(nx(2), b0))
    arrived(f3, rows_b(nx(2), b1))

    def squares(i, total):
        v = xg[i // 4, lax.rem(i, 4)].astype(F32)
        v = v * v
        return total + (v[:, 0:128] + v[:, 128:256])

    with jax.named_scope("squares"):
        total = lax.fori_loop(0, 16, squares, jnp.zeros((256, 128), F32))
        scale = lax.rsqrt(jnp.sum(total, axis=1, keepdims=True) * (1.0 / 4096) + EPS)
    ring(5)

    def normalise(i, carry):
        v = xg[i // 4, lax.rem(i, 4)].astype(F32)
        n = (v * scale).astype(BF16)
        xn[i] = n
        xm[i] = dot(chosen, n).astype(BF16)
        return carry

    with jax.named_scope("normalise"):
        lax.fori_loop(0, 16, normalise, 0)

    def project(m, *distances):
        take(m, *distances)
        if m == K:
            take(B, *distances)
        acc = {Q: acc_q, V: acc_v, K: acc_k}[m]
        left = xn if m == Q else xm
        for d in distances:
            i = nz(d) * 2
            acc[...] += dot(left[i], bufs[m][i]) + dot(left[i + 1], bufs[m][i + 1])
            if m == K:
                logits[...] += dot(left[i], gb[i], NT) + dot(left[i + 1], gb[i + 1], NT)

    ring(6)
    with jax.named_scope("project_q"):
        project(Q, 0, -1, 1, -2, 2)
    ring(7, 8, 9, 10)
    project(Q, -3, 3, 4)

    def wide_state(h):
        high, lo = split(state[h])
        return jnp.concatenate([high, lo, high], axis=1)

    def through(rows, wide):
        high, lo = split(rows)
        return dot(jnp.concatenate([high, high, lo], axis=1), wide, NT)

    cols = (slice(0, 128), slice(128, 256))
    seg_rows = (slice(0, 128), slice(128, 256))
    seg_mem = (slice(0, 64), slice(64, 128))

    def queries(seg, h):
        return acc_q[seg_rows[seg], cols[h]] * (128.0 ** -0.5)

    wides = [wide_state(h) for h in range(2)]
    for h in range(2):
        base[:, cols[h]] = through(queries(1, h), wides[h])
    readout = jnp.concatenate([through(queries(0, h), wides[h]) for h in range(2)], axis=1).astype(BF16)
    take(O, 0, -1, 1, -2, 2, -3, 3, 4)
    scatter = [
        Scatter(net, [r.at[seg] for r in sums], (nx, ny), (xp, xd, x2, yp, yd, y2)) for seg in range(2)
    ]
    with jax.named_scope("multiply0"):
        scatter[0].start(readout, go)
        scatter[0].push(False)
    project(K, 0, -1, 1)
    ring(11, 12)
    scatter[0].hand_on()
    ring(13)
    project(V, 0, -1, 1)
    ring(14)
    project(K, -2, 2)
    ring(15)
    project(V, -2, 2)
    ring(16)
    project(K, -3, 3)
    scatter[0].turn()
    project(V, -3, 3)
    project(K, 4)

    keys, betas, recalls, matches = [], [], [], []
    with jax.named_scope("prepare"):
        for h in range(2):
            k = acc_k[:, cols[h]]
            k = k * lax.rsqrt(jnp.sum(k * k, axis=1, keepdims=True) + 1e-06)
            keys.append(k)
            betas.append(jax.nn.sigmoid(logits[:, h:h + 1]))
            kh, kl = split(k[seg_mem[0]])
            match_high, match_low = split(through(queries(1, h), jnp.concatenate([kh, kl, kh], axis=1)))
            matches.append(jnp.concatenate([match_high, match_high, match_low], axis=1))
            recalls.append(through(k[seg_mem[0]], wide_state(h)))
    ring(17)
    project(V, 4)
    values = [acc_v[:, cols[h]] for h in range(2)]

    def change(seg, h, recalled):
        m = seg_mem[seg]
        return split(betas[h][m] * (values[h][m] - recalled))

    def update(seg, h, changed):
        ch, cl = changed
        kh, kl = split(keys[h][seg_mem[seg]])
        state[h] += dot(jnp.concatenate([ch, ch, cl], axis=0), jnp.concatenate([kh, kl, kh], axis=0), TN)

    with jax.named_scope("recur"):
        changes, readouts = [], []
        for h in range(2):
            ch, cl = change(0, h, recalls[h])
            changes.append((ch, cl))
            readouts.append(base[:, cols[h]] + dot(matches[h], jnp.concatenate([ch, cl, ch], axis=0)))
        readout = jnp.concatenate(readouts, axis=1).astype(BF16)
    with jax.named_scope("multiply1"):
        scatter[1].start(readout, go)

    for h in range(2):
        update(0, h, changes[h])
        update(1, h, change(1, h, through(keys[h][seg_mem[1]], wide_state(h))))
    scatter[1].push(True)
    stored = []
    for h in range(2):
        copy = pltpu.make_async_copy(state.at[h], memory_ref.at[0, h], local.at[h])
        copy.start()
        stored.append(copy)

    def put_out(seg):
        for part in scatter[seg].last(xg.at[y, x], out_v, seg * 128):
            copy = pltpu.make_async_copy(out_v.at[part], out_ref.at[0, part], local.at[len(stored)])
            copy.start()
            stored.append(copy)

    scatter[1].hand_on()
    put_out(0)
    scatter[1].turn()
    with jax.named_scope("drain"):
        net.drain()
    put_out(1)
    with jax.named_scope("stored"):
        for copy in stored:
            copy.wait()


COPIES = 151


def finish(hidden_in, memory_in, hidden_out, memory_out, hidden, memory):
    def run(arrive, leave):
        moves = []
        for i in range(2):
            rows = slice(128 * i, 128 * i + 128)
            moves.append((hidden_in.at[0, rows], hidden.at[rows], hidden_out.at[0, rows]))
            moves.append((memory_in.at[0, i], memory.at[i], memory_out.at[0, i]))
        first = [pltpu.make_async_copy(src, via, arrive.at[i]) for i, (src, via, _) in enumerate(moves)]
        second = [pltpu.make_async_copy(via, dst, leave.at[i]) for i, (_, via, dst) in enumerate(moves)]
        for copy in first:
            copy.start()
        for before, after in zip(first, second):
            before.wait()
            after.start()
        for copy in second:
            copy.wait()

    pl.run_scoped(run, pltpu.SemaphoreType.DMA((4,)), pltpu.SemaphoreType.DMA((4,)))


def body(hidden_in, w_query, w_key, w_value, w_beta, w_out, mem_pos, memory_in):
    vmem = pltpu.VMEM
    scratch = [
        vmem((4, 4, 256, 256), BF16),
        vmem((16, 256, 256), BF16),
        vmem((16, 128, 256), BF16),
        vmem((16, 256, 256), BF16),
        vmem((16, 256, 256), BF16),
        vmem((16, 256, 256), BF16),
        vmem((16, 256, 256), BF16),
        vmem((16, 2, 256), BF16),
        vmem((2, 64), jnp.int32),
        vmem((2, 128, 128), F32),
        vmem((256, 256), BF16),
        vmem((256, 256), F32),
        vmem((128, 256), F32),
        vmem((128, 256), F32),
        vmem((128, 256), F32),
        vmem((128, 2), F32),
        vmem((2, 4, 4, 64, 256), BF16),
        vmem((2, 2, 4, 32, 256), BF16),
        vmem((2, 2, 4, 32, 256), BF16),
        vmem((2, 2, 4, 64, 256), BF16),
        vmem((2, 3, 64, 256), BF16),
        vmem((2, 64, 256), F32),
        vmem((2, 3, 64, 256), BF16),
        vmem((2, 4, 4, 64, 256), BF16),
        vmem((2, 2, 4, 32, 256), BF16),
        vmem((2, 2, 4, 32, 256), BF16),
        vmem((2, 2, 4, 64, 256), BF16),
        vmem((2, 3, 64, 256), BF16),
        vmem((2, 64, 256), F32),
        vmem((2, 3, 64, 256), BF16),
    ]
    results = pl.pallas_call(
        kernel,
        out_shape=(
            jax.ShapeDtypeStruct(hidden_in.shape, BF16),
            jax.ShapeDtypeStruct(memory_in.shape, F32),
        ),
        in_specs=[pl.BlockSpec(memory_space=pltpu.HBM)] * 8,
        out_specs=[pl.BlockSpec(memory_space=pltpu.HBM)] * 2,
        scratch_shapes=scratch,
        compiler_params=pltpu.CompilerParams(
            collective_id=0, has_side_effects=True
        ),
    )(hidden_in, w_query, w_key, w_value, w_beta.T, w_out, mem_pos, memory_in)
    return pl.pallas_call(
        finish,
        out_shape=[jax.ShapeDtypeStruct(r.shape, r.dtype) for r in results],
        in_specs=[pl.BlockSpec(memory_space=pltpu.HBM)] * 2,
        out_specs=[pl.BlockSpec(memory_space=pltpu.HBM)] * 2,
        scratch_shapes=[vmem((256, 256), BF16), vmem((2, 128, 128), F32)],
    )(*results)


def solution(mesh):
    split = Mesh(mesh.devices.reshape(4, 4, 8, 2), ("y", "x", "z", "c"))
    return jax.shard_map(
        body,
        mesh=split,
        in_specs=(
            P(BATCH, None, HEAD),
            P(BATCH, HEAD),
            P(BATCH, HEAD),
            P(BATCH, HEAD),
            P(BATCH, HEAD),
            P(HEAD, BATCH),
            P(BATCH, None, None),
            P(BATCH, HEAD, None, None),
        ),
        out_specs=(P(BATCH, None, HEAD), P(BATCH, HEAD, None, None)),
        check_vma=False,
    )
```

```python
import functools

import jax
import jax.numpy as jnp
from jax import lax
from jax.experimental import pallas as pl
from jax.experimental.pallas import tpu as pltpu
from jax.sharding import Mesh
from jax.sharding import PartitionSpec as P

HEAD = ("y", "x")
BATCH = ("z", "c")
EPS = 1e-05
F32 = jnp.float32
BF16 = jnp.bfloat16
HIGHEST = lax.Precision.HIGHEST
NN = (((1,), (0,)), ((), ()))
NT = (((1,), (1,)), ((), ()))
TN = (((0,), (0,)), ((), ()))


def dot(a, b, dims=NN, precision=None):
    return lax.dot_general(a, b, dims, precision=precision, preferred_element_type=F32)


class Copies:
    def __init__(self, send, recv):
        self.send, self.recv, self.count, self.sent = send, recv, 0, {}

    def post(self, src, dst, to):
        slot = self.count
        self.count += 1
        copy = pltpu.make_async_remote_copy(
            src_ref=src,
            dst_ref=dst,
            send_sem=self.send.at[slot],
            recv_sem=self.recv.at[slot],
            device_id=to,
            device_id_type=pl.DeviceIdType.MESH,
        )
        copy.start()
        self.sent[slot] = copy
        return slot

    def same(self, ref, to):
        return self.post(ref, ref, to)

    def arrived(self, slot, ref):
        pltpu.make_async_copy(ref, ref, self.recv.at[slot]).wait()

    def gone(self, slot):
        self.sent.pop(slot).wait_send()

    def drain(self):
        for slot in tuple(self.sent):
            self.gone(slot)


class Scatter:
    HOPS = (2, 1, 3, 0)

    def __init__(self, net, refs, steps, peers):
        self.net, self.steps = net, steps
        self.sides = tuple(zip((refs[:7], refs[7:]), (peers[:3], peers[3:]), (peers[3:], peers[:3])))

    def multiply(self, rows, weights, hops):
        (pa, *_), (pb, *_) = (side[0] for side in self.sides)
        nx, ny = self.steps
        for dy in range(4):
            for dx in range(4):
                if max((0, 1, 2, 1)[dx], (0, 1, 2, 1)[dy]) == hops:
                    got = dot(rows, weights[ny(dy) * 4 + nx(dx)]).astype(BF16)
                    pa[dx, self.HOPS.index(dy)] = got[0:64]
                    pb[dy, self.HOPS.index(dx)] = got[64:128]

    def start(self, rows, weights):
        self.multiply(rows, weights, 2)
        self.h = []
        for (p, half, *_), to, _ in self.sides:
            for i in range(2):
                self.h.append(self.net.post(p.at[2, :, 32 * i:32 * i + 32], half.at[i], to[i]))
        self.multiply(rows, weights, 1)
        self.multiply(rows, weights, 0)

    def push(self, wait):
        if wait:
            for slot in self.h:
                self.net.gone(slot)
        self.f = []
        for part in (slice(0, 1), slice(1, 4)):
            for (p, _, _, full, *_), to, _ in self.sides:
                for i in range(2):
                    self.f.append(self.net.post(p.at[1 + 2 * i, part], full.at[i, part], to[i]))

    def hand_on(self):
        early, late = [], []
        for j, ((_, half, far, *_), to, _) in enumerate(self.sides):
            for i in range(2):
                self.net.arrived(self.h[2 * j + i], half.at[i])
                early.append(self.net.post(half.at[i, 0:1], far.at[i, 0:1], to[i]))
                late.append(self.net.post(half.at[i, 1:4], far.at[i, 1:4], to[i]))
        self.h = early + late

    def turn(self):
        self.e = [[], []]
        for late, part in enumerate((slice(0, 1), slice(1, 4))):
            for j, ((p, _, far, full, total, own, end), _, peers) in enumerate(self.sides):
                for i in range(2):
                    self.net.arrived(self.f[4 * late + 2 * j + i], full.at[i, part])
                near = p[0, part].astype(F32) + full[0, part].astype(F32) + full[1, part].astype(F32)
                for i in range(2):
                    self.net.arrived(self.h[4 * late + 2 * j + i], far.at[i, part])
                passed = jnp.concatenate([far[0, part].astype(F32), far[1, part].astype(F32)], axis=1)
                near = near + passed
                if late:
                    total[1:3] = near[0:2].astype(BF16)
                    own[...] = near[2]
                    self.e[j].append(self.net.post(total.at[1], end.at[1], peers[0]))
                    self.e[j].append(self.net.post(total.at[2], end.at[2], peers[1]))
                else:
                    total[0:1] = near.astype(BF16)
                    self.e[j].append(self.net.post(total.at[0], end.at[0], peers[2]))

    def last(self, residual, out, start):
        for j, ((*_, own, end), _, _) in enumerate(self.sides):
            mixed = own[...]
            for i in range(3):
                self.net.arrived(self.e[j][i], end.at[i])
                mixed += end[i].astype(F32)
            rows = slice(start + j * 64, start + j * 64 + 64)
            out[rows] = (residual[rows].astype(F32) + mixed).astype(BF16)
            yield rows


def split(v):
    high = v.astype(BF16)
    return high, (v - high.astype(F32)).astype(BF16)


def kernel(*refs):
    dma = pltpu.SemaphoreType.DMA
    pl.run_scoped(functools.partial(layer, *refs), dma((8,)), dma((COPIES,)), dma((COPIES,)))


def layer(
    x_in, wq_in, wk_in, wv_in, wb_in, wo_in, pos_in, mem_in,
    out_ref, memory_ref,
    xg, xn, xm, gv, gq, gk, go, gb, pos_v, state, out_v,
    acc_q, acc_k, acc_v, base, logits, *rest,
):
    sums, (local, send, recv) = rest[:-3], rest[-3:]
    y, x, z, c = (lax.axis_index(n) for n in ("y", "x", "z", "c"))
    ny = lambda d: lax.rem(y + (d % 4), 4)
    nx = lambda d: lax.rem(x + (d % 4), 4)
    nz = lambda d: lax.rem(z + (d % 8), 8)
    up, down = {"z": nz(1)}, {"z": nz(-1)}
    xp, xd = {"x": nx(1)}, {"x": nx(-1)}
    yp, yd = {"y": ny(1)}, {"y": ny(-1)}
    partner = {"c": 1 - c}
    mine = z * 2 + c

    barrier = pltpu.get_barrier_semaphore()
    x2, y2 = {"x": nx(2)}, {"y": ny(2)}
    for peer in (up, down, xp, xd, yp, yd, x2, y2, partner):
        pl.semaphore_signal(barrier, inc=1, device_id=peer, device_id_type=pl.DeviceIdType.MESH)

    loads = [
        (x_in.at[0], xg.at[y, x]),
        (wq_in, gq.at[mine]),
        (wo_in, go.at[mine]),
        (wb_in, gb.at[mine]),
        (wk_in, gk.at[mine]),
        (wv_in, gv.at[mine]),
        (pos_in.at[0], pos_v),
        (mem_in.at[0], state),
    ]
    fetched = []
    for i, (src, dst) in enumerate(loads):
        copy = pltpu.make_async_copy(src, dst, local.at[i])
        copy.start()
        fetched.append(copy)
    fetched[0].wait()
    with jax.named_scope("enter"):
        pl.semaphore_wait(barrier, 9)
    net = Copies(send, recv)
    same, arrived = net.same, net.arrived

    a0, a1, b0, b1 = slice(0, 64), slice(64, 128), slice(128, 192), slice(192, 256)
    top, low = slice(0, 128), slice(128, 256)

    from_down, from_up, from_partner = {}, {}, {}
    Q, O, V, K, B = range(5)
    bufs = (gq, go, gv, gk, gb)
    order = (
        (Q, 0), (O, 0), (K, 0), (Q, 1), (O, 1), (V, 0), (Q, 2), (O, 2), (K, 1), (Q, 3), (O, 3), (V, 1),
        (K, 2, 0), (K, 2, 1), (V, 2, 0), (V, 2, 1), (K, 3), (V, 3),
    )
    leave = {0: 3, 1: 4, 2: 5, 3: 6, 4: 7, 5: 8, 6: 9, 7: 10, 8: 11, 9: 12, 10: 13, 11: 14, 12: 15, 13: 16, 14: 17}

    def block(d):
        return nz(d) * 2 + c

    def give(m, *distances):
        for d in distances:
            from_partner[m, d] = same(bufs[m].at[block(d)], partner)

    def pieces(m, s, later=None):
        if s < 3 and later is None:
            return slice(None), slice(None)
        return (low, top) if later else (top, low)

    def issue(i):
        m, s = order[i][:2]
        ahead, behind = pieces(*order[i])
        from_down[i] = same(bufs[m].at[block(-s), ahead], up)
        from_up[i] = same(bufs[m].at[block(s), behind], down)
        if m == K and order[i][2:] != (1,):
            from_down[B, s] = same(gb.at[block(-s)], up)
            if s < 3:
                from_up[B, s] = same(gb.at[block(s)], down)

    def ring(*indices):
        for i in indices:
            m, s, *later = order[i]
            ahead, behind = pieces(*order[i])
            arrived(from_down[i], bufs[m].at[block(-s - 1), ahead])
            arrived(from_up[i], bufs[m].at[block(s + 1), behind])
            if m == K and later != [1]:
                arrived(from_down[B, s], gb.at[block(-s - 1)])
                if s < 3:
                    arrived(from_up[B, s], gb.at[block(s + 1)])
            if i in leave:
                issue(leave[i])
            if m == K and later != [1]:
                give(B, *((-s - 1, s + 1) if s < 3 else (4,)))
            if s == 3:
                give(m, 4)
            elif later != [0]:
                give(m, -s - 1, s + 1)

    def take(m, *distances):
        for d in distances:
            arrived(from_partner[m, d], bufs[m].at[nz(d) * 2 + (1 - c)])

    own_a, own_b = xg.at[y, x, top], xg.at[y, x, low]
    for i, needs in enumerate(((1,), (2,), (3, 4))):
        for j in needs:
            fetched[j].wait()
        issue(i)
        if i == 0:
            s = [same(own_a, xp), same(own_a, xd), same(own_b, yp), same(own_b, yd)]
    for copy in fetched[5:]:
        copy.wait()
    acc_q[...] = jnp.zeros_like(acc_q)
    acc_k[...] = jnp.zeros_like(acc_k)
    acc_v[...] = jnp.zeros_like(acc_v)
    logits[...] = jnp.zeros_like(logits)
    row = lax.broadcasted_iota(jnp.int32, (256, 128), 0)
    where = jnp.concatenate([pos_v[0:1, :], pos_v[1:2, :] + 128], axis=1)
    chosen = jnp.where(row == where, 1.0, 0.0).T.astype(BF16)

    arrived(s[0], xg.at[y, nx(-1), top])
    f0 = same(xg.at[y, nx(-1), a0], xp)
    arrived(s[1], xg.at[y, nx(1), top])
    f1 = same(xg.at[y, nx(1), a1], xd)
    arrived(s[2], xg.at[ny(-1), x, low])
    f2 = same(xg.at[ny(-1), x, b0], yp)
    arrived(s[3], xg.at[ny(1), x, low])
    f3 = same(xg.at[ny(1), x, b1], yd)
    arrived(f0, xg.at[y, nx(2), a0])
    arrived(f1, xg.at[y, nx(2), a1])
    rows_a = lambda yy, r: xg.at[yy, :, r]
    s0 = same(rows_a(y, top), yp)
    s1 = same(rows_a(y, top), yd)
    arrived(f2, xg.at[ny(2), x, b0])
    arrived(f3, xg.at[ny(2), x, b1])
    rows_b = lambda xx, r: xg.at[:, xx, r]
    s2 = same(rows_b(x, low), xp)
    s3 = same(rows_b(x, low), xd)
    ring(0, 1, 2)

    arrived(s0, rows_a(ny(-1), top))
    f0 = same(rows_a(ny(-1), a0), yp)
    arrived(s1, rows_a(ny(1), top))
    f1 = same(rows_a(ny(1), a1), yd)
    arrived(s2, rows_b(nx(-1), low))
    f2 = same(rows_b(nx(-1), b0), xp)
    arrived(s3, rows_b(nx(1), low))
    f3 = same(rows_b(nx(1), b1), xd)
    ring(3, 4)
    for m in (Q, O, V, K, B):
        give(m, 0)
    arrived(f0, rows_a(ny(2), a0))
    arrived(f1, rows_a(ny(2), a1))
    arrived(f2, rows_b(nx(2), b0))
    arrived(f3, rows_b(nx(2), b1))

    def squares(i, total):
        v = xg[i // 4, lax.rem(i, 4)].astype(F32)
        v = v * v
        return total + (v[:, 0:128] + v[:, 128:256])

    with jax.named_scope("squares"):
        total = lax.fori_loop(0, 16, squares, jnp.zeros((256, 128), F32))
        scale = lax.rsqrt(jnp.sum(total, axis=1, keepdims=True) * (1.0 / 4096) + EPS)
    ring(5)

    def normalise(i, carry):
        v = xg[i // 4, lax.rem(i, 4)].astype(F32)
        n = (v * scale).astype(BF16)
        xn[i] = n
        xm[i] = dot(chosen, n).astype(BF16)
        return carry

    with jax.named_scope("normalise"):
        lax.fori_loop(0, 16, normalise, 0)

    def project(m, *distances):
        take(m, *distances)
        if m == K:
            take(B, *distances)
        acc = {Q: acc_q, V: acc_v, K: acc_k}[m]
        left = xn if m == Q else xm
        for d in distances:
            i = nz(d) * 2
            acc[...] += dot(left[i], bufs[m][i]) + dot(left[i + 1], bufs[m][i + 1])
            if m == K:
                logits[...] += dot(left[i], gb[i], NT) + dot(left[i + 1], gb[i + 1], NT)

    ring(6)
    with jax.named_scope("project_q"):
        project(Q, 0, -1, 1, -2, 2)
    ring(7, 8, 9, 10)
    project(Q, -3, 3, 4)

    def wide_state(h):
        high, lo = split(state[h])
        return jnp.concatenate([high, lo, high], axis=1)

    def through(rows, wide):
        high, lo = split(rows)
        return dot(jnp.concatenate([high, high, lo], axis=1), wide, NT)

    cols = (slice(0, 128), slice(128, 256))
    seg_rows = (slice(0, 128), slice(128, 256))
    seg_mem = (slice(0, 64), slice(64, 128))

    def queries(seg, h):
        return acc_q[seg_rows[seg], cols[h]] * (128.0 ** -0.5)

    wides = [wide_state(h) for h in range(2)]
    for h in range(2):
        base[:, cols[h]] = through(queries(1, h), wides[h])
    readout = jnp.concatenate([through(queries(0, h), wides[h]) for h in range(2)], axis=1).astype(BF16)
    take(O, 0, -1, 1, -2, 2, -3, 3, 4)
    scatter = [
        Scatter(net, [r.at[seg] for r in sums], (nx, ny), (xp, xd, x2, yp, yd, y2)) for seg in range(2)
    ]
    with jax.named_scope("multiply0"):
        scatter[0].start(readout, go)
        scatter[0].push(False)
    project(K, 0, -1, 1)
    ring(11, 12)
    scatter[0].hand_on()
    ring(13)
    project(V, 0, -1, 1)
    ring(14)
    project(K, -2, 2)
    ring(15)
    project(V, -2, 2)
    ring(16)
    project(K, -3, 3)
    scatter[0].turn()
    project(V, -3, 3)
    project(K, 4)

    keys, betas, recalls, matches = [], [], [], []
    with jax.named_scope("prepare"):
        for h in range(2):
            k = acc_k[:, cols[h]]
            k = k * lax.rsqrt(jnp.sum(k * k, axis=1, keepdims=True) + 1e-06)
            keys.append(k)
            betas.append(jax.nn.sigmoid(logits[:, h:h + 1]))
            kh, kl = split(k[seg_mem[0]])
            match_high, match_low = split(through(queries(1, h), jnp.concatenate([kh, kl, kh], axis=1)))
            matches.append(jnp.concatenate([match_high, match_high, match_low], axis=1))
            recalls.append(through(k[seg_mem[0]], wide_state(h)))
    ring(17)
    project(V, 4)
    values = [acc_v[:, cols[h]] for h in range(2)]

    def change(seg, h, recalled):
        m = seg_mem[seg]
        return split(betas[h][m] * (values[h][m] - recalled))

    def update(seg, h, changed):
        ch, cl = changed
        kh, kl = split(keys[h][seg_mem[seg]])
        state[h] += dot(jnp.concatenate([ch, ch, cl], axis=0), jnp.concatenate([kh, kl, kh], axis=0), TN)

    with jax.named_scope("recur"):
        changes, readouts = [], []
        for h in range(2):
            ch, cl = change(0, h, recalls[h])
            changes.append((ch, cl))
            readouts.append(base[:, cols[h]] + dot(matches[h], jnp.concatenate([ch, cl, ch], axis=0)))
        readout = jnp.concatenate(readouts, axis=1).astype(BF16)
    with jax.named_scope("multiply1"):
        scatter[1].start(readout, go)

    for h in range(2):
        update(0, h, changes[h])
    scatter[1].push(True)
    for h in range(2):
        update(1, h, change(1, h, through(keys[h][seg_mem[1]], wide_state(h))))
    stored = []
    for h in range(2):
        copy = pltpu.make_async_copy(state.at[h], memory_ref.at[0, h], local.at[h])
        copy.start()
        stored.append(copy)

    def put_out(seg):
        for part in scatter[seg].last(xg.at[y, x], out_v, seg * 128):
            copy = pltpu.make_async_copy(out_v.at[part], out_ref.at[0, part], local.at[len(stored)])
            copy.start()
            stored.append(copy)

    scatter[1].hand_on()
    put_out(0)
    scatter[1].turn()
    with jax.named_scope("drain"):
        net.drain()
    put_out(1)
    with jax.named_scope("stored"):
        for copy in stored:
            copy.wait()


COPIES = 151


def finish(hidden_in, memory_in, hidden_out, memory_out, hidden, memory):
    def run(arrive, leave):
        moves = []
        for i in range(2):
            rows = slice(128 * i, 128 * i + 128)
            moves.append((hidden_in.at[0, rows], hidden.at[rows], hidden_out.at[0, rows]))
            moves.append((memory_in.at[0, i], memory.at[i], memory_out.at[0, i]))
        first = [pltpu.make_async_copy(src, via, arrive.at[i]) for i, (src, via, _) in enumerate(moves)]
        second = [pltpu.make_async_copy(via, dst, leave.at[i]) for i, (_, via, dst) in enumerate(moves)]
        for copy in first:
            copy.start()
        for before, after in zip(first, second):
            before.wait()
            after.start()
        for copy in second:
            copy.wait()

    pl.run_scoped(run, pltpu.SemaphoreType.DMA((4,)), pltpu.SemaphoreType.DMA((4,)))


def body(hidden_in, w_query, w_key, w_value, w_beta, w_out, mem_pos, memory_in):
    vmem = pltpu.VMEM
    scratch = [
        vmem((4, 4, 256, 256), BF16),
        vmem((16, 256, 256), BF16),
        vmem((16, 128, 256), BF16),
        vmem((16, 256, 256), BF16),
        vmem((16, 256, 256), BF16),
        vmem((16, 256, 256), BF16),
        vmem((16, 256, 256), BF16),
        vmem((16, 2, 256), BF16),
        vmem((2, 64), jnp.int32),
        vmem((2, 128, 128), F32),
        vmem((256, 256), BF16),
        vmem((256, 256), F32),
        vmem((128, 256), F32),
        vmem((128, 256), F32),
        vmem((128, 256), F32),
        vmem((128, 2), F32),
        vmem((2, 4, 4, 64, 256), BF16),
        vmem((2, 2, 4, 32, 256), BF16),
        vmem((2, 2, 4, 32, 256), BF16),
        vmem((2, 2, 4, 64, 256), BF16),
        vmem((2, 3, 64, 256), BF16),
        vmem((2, 64, 256), F32),
        vmem((2, 3, 64, 256), BF16),
        vmem((2, 4, 4, 64, 256), BF16),
        vmem((2, 2, 4, 32, 256), BF16),
        vmem((2, 2, 4, 32, 256), BF16),
        vmem((2, 2, 4, 64, 256), BF16),
        vmem((2, 3, 64, 256), BF16),
        vmem((2, 64, 256), F32),
        vmem((2, 3, 64, 256), BF16),
    ]
    results = pl.pallas_call(
        kernel,
        out_shape=(
            jax.ShapeDtypeStruct(hidden_in.shape, BF16),
            jax.ShapeDtypeStruct(memory_in.shape, F32),
        ),
        in_specs=[pl.BlockSpec(memory_space=pltpu.HBM)] * 8,
        out_specs=[pl.BlockSpec(memory_space=pltpu.HBM)] * 2,
        scratch_shapes=scratch,
        compiler_params=pltpu.CompilerParams(
            collective_id=0, has_side_effects=True
        ),
    )(hidden_in, w_query, w_key, w_value, w_beta.T, w_out, mem_pos, memory_in)
    return pl.pallas_call(
        finish,
        out_shape=[jax.ShapeDtypeStruct(r.shape, r.dtype) for r in results],
        in_specs=[pl.BlockSpec(memory_space=pltpu.HBM)] * 2,
        out_specs=[pl.BlockSpec(memory_space=pltpu.HBM)] * 2,
        scratch_shapes=[vmem((256, 256), BF16), vmem((2, 128, 128), F32)],
    )(*results)


def solution(mesh):
    split = Mesh(mesh.devices.reshape(4, 4, 8, 2), ("y", "x", "z", "c"))
    return jax.shard_map(
        body,
        mesh=split,
        in_specs=(
            P(BATCH, None, HEAD),
            P(BATCH, HEAD),
            P(BATCH, HEAD),
            P(BATCH, HEAD),
            P(BATCH, HEAD),
            P(HEAD, BATCH),
            P(BATCH, None, None),
            P(BATCH, HEAD, None, None),
        ),
        out_specs=(P(BATCH, None, HEAD), P(BATCH, HEAD, None, None)),
        check_vma=False,
    )
```

```python
import functools

import jax
import jax.numpy as jnp
from jax import lax
from jax.experimental import pallas as pl
from jax.experimental.pallas import tpu as pltpu
from jax.sharding import Mesh
from jax.sharding import PartitionSpec as P

HEAD = ("y", "x")
BATCH = ("z", "c")
EPS = 1e-05
F32 = jnp.float32
BF16 = jnp.bfloat16
HIGHEST = lax.Precision.HIGHEST
NN = (((1,), (0,)), ((), ()))
NT = (((1,), (1,)), ((), ()))
TN = (((0,), (0,)), ((), ()))


def dot(a, b, dims=NN, precision=None):
    return lax.dot_general(a, b, dims, precision=precision, preferred_element_type=F32)


class Copies:
    def __init__(self, send, recv):
        self.send, self.recv, self.count, self.sent = send, recv, 0, {}

    def post(self, src, dst, to):
        slot = self.count
        self.count += 1
        copy = pltpu.make_async_remote_copy(
            src_ref=src,
            dst_ref=dst,
            send_sem=self.send.at[slot],
            recv_sem=self.recv.at[slot],
            device_id=to,
            device_id_type=pl.DeviceIdType.MESH,
        )
        copy.start()
        self.sent[slot] = copy
        return slot

    def same(self, ref, to):
        return self.post(ref, ref, to)

    def arrived(self, slot, ref):
        pltpu.make_async_copy(ref, ref, self.recv.at[slot]).wait()

    def gone(self, slot):
        self.sent.pop(slot).wait_send()

    def drain(self):
        for slot in tuple(self.sent):
            self.gone(slot)


class Scatter:
    HOPS = (2, 1, 3, 0)

    def __init__(self, net, refs, steps, peers):
        self.net, self.steps = net, steps
        self.sides = tuple(zip((refs[:7], refs[7:]), (peers[:3], peers[3:]), (peers[3:], peers[:3])))

    def multiply(self, rows, weights, hops):
        (pa, *_), (pb, *_) = (side[0] for side in self.sides)
        nx, ny = self.steps
        for dy in range(4):
            for dx in range(4):
                if max((0, 1, 2, 1)[dx], (0, 1, 2, 1)[dy]) == hops:
                    got = dot(rows, weights[ny(dy) * 4 + nx(dx)]).astype(BF16)
                    pa[dx, self.HOPS.index(dy)] = got[0:64]
                    pb[dy, self.HOPS.index(dx)] = got[64:128]

    def start(self, rows, weights):
        self.multiply(rows, weights, 2)
        self.h = []
        for (p, half, *_), to, _ in self.sides:
            for i in range(2):
                self.h.append(self.net.post(p.at[2, :, 32 * i:32 * i + 32], half.at[i], to[i]))
        self.f = []
        self.near(slice(0, 1))
        self.multiply(rows, weights, 1)
        self.multiply(rows, weights, 0)

    def near(self, part):
        for (p, _, _, full, *_), to, _ in self.sides:
            for i in range(2):
                self.f.append(self.net.post(p.at[1 + 2 * i, part], full.at[i, part], to[i]))

    def push(self, wait):
        if wait:
            for slot in self.h:
                self.net.gone(slot)
        self.near(slice(1, 4))

    def hand_on(self):
        early, late = [], []
        for j, ((_, half, far, *_), to, _) in enumerate(self.sides):
            for i in range(2):
                self.net.arrived(self.h[2 * j + i], half.at[i])
                early.append(self.net.post(half.at[i, 0:1], far.at[i, 0:1], to[i]))
                late.append(self.net.post(half.at[i, 1:4], far.at[i, 1:4], to[i]))
        self.h = early + late

    def turn(self):
        self.e = [[], []]
        for late, part in enumerate((slice(0, 1), slice(1, 4))):
            for j, ((p, _, far, full, total, own, end), _, peers) in enumerate(self.sides):
                for i in range(2):
                    self.net.arrived(self.f[4 * late + 2 * j + i], full.at[i, part])
                near = p[0, part].astype(F32) + full[0, part].astype(F32) + full[1, part].astype(F32)
                for i in range(2):
                    self.net.arrived(self.h[4 * late + 2 * j + i], far.at[i, part])
                passed = jnp.concatenate([far[0, part].astype(F32), far[1, part].astype(F32)], axis=1)
                near = near + passed
                if late:
                    total[1:3] = near[0:2].astype(BF16)
                    own[...] = near[2]
                    self.e[j].append(self.net.post(total.at[1], end.at[1], peers[0]))
                    self.e[j].append(self.net.post(total.at[2], end.at[2], peers[1]))
                else:
                    total[0:1] = near.astype(BF16)
                    self.e[j].append(self.net.post(total.at[0], end.at[0], peers[2]))

    def last(self, residual, out, start):
        for j, ((*_, own, end), _, _) in enumerate(self.sides):
            mixed = own[...]
            for i in range(3):
                self.net.arrived(self.e[j][i], end.at[i])
                mixed += end[i].astype(F32)
            rows = slice(start + j * 64, start + j * 64 + 64)
            out[rows] = (residual[rows].astype(F32) + mixed).astype(BF16)
            yield rows


def split(v):
    high = v.astype(BF16)
    return high, (v - high.astype(F32)).astype(BF16)


def kernel(*refs):
    dma = pltpu.SemaphoreType.DMA
    pl.run_scoped(functools.partial(layer, *refs), dma((8,)), dma((COPIES,)), dma((COPIES,)))


def layer(
    x_in, wq_in, wk_in, wv_in, wb_in, wo_in, pos_in, mem_in,
    out_ref, memory_ref,
    xg, xn, xm, gv, gq, gk, go, gb, pos_v, state, out_v,
    acc_q, acc_k, acc_v, base, logits, *rest,
):
    sums, (local, send, recv) = rest[:-3], rest[-3:]
    y, x, z, c = (lax.axis_index(n) for n in ("y", "x", "z", "c"))
    ny = lambda d: lax.rem(y + (d % 4), 4)
    nx = lambda d: lax.rem(x + (d % 4), 4)
    nz = lambda d: lax.rem(z + (d % 8), 8)
    up, down = {"z": nz(1)}, {"z": nz(-1)}
    xp, xd = {"x": nx(1)}, {"x": nx(-1)}
    yp, yd = {"y": ny(1)}, {"y": ny(-1)}
    partner = {"c": 1 - c}
    mine = z * 2 + c

    barrier = pltpu.get_barrier_semaphore()
    x2, y2 = {"x": nx(2)}, {"y": ny(2)}
    for peer in (up, down, xp, xd, yp, yd, x2, y2, partner):
        pl.semaphore_signal(barrier, inc=1, device_id=peer, device_id_type=pl.DeviceIdType.MESH)

    loads = [
        (x_in.at[0], xg.at[y, x]),
        (wq_in, gq.at[mine]),
        (wo_in, go.at[mine]),
        (wb_in, gb.at[mine]),
        (wk_in, gk.at[mine]),
        (wv_in, gv.at[mine]),
        (pos_in.at[0], pos_v),
        (mem_in.at[0], state),
    ]
    fetched = []
    for i, (src, dst) in enumerate(loads):
        copy = pltpu.make_async_copy(src, dst, local.at[i])
        copy.start()
        fetched.append(copy)
    fetched[0].wait()
    with jax.named_scope("enter"):
        pl.semaphore_wait(barrier, 9)
    net = Copies(send, recv)
    same, arrived = net.same, net.arrived

    a0, a1, b0, b1 = slice(0, 64), slice(64, 128), slice(128, 192), slice(192, 256)
    top, low = slice(0, 128), slice(128, 256)

    from_down, from_up, from_partner = {}, {}, {}
    Q, O, V, K, B = range(5)
    bufs = (gq, go, gv, gk, gb)
    order = (
        (Q, 0), (O, 0), (K, 0), (Q, 1), (O, 1), (V, 0), (Q, 2), (O, 2), (K, 1), (Q, 3), (O, 3), (V, 1),
        (K, 2, 0), (K, 2, 1), (V, 2, 0), (V, 2, 1), (K, 3), (V, 3),
    )
    leave = {0: 3, 1: 4, 2: 5, 3: 6, 4: 7, 5: 8, 6: 9, 7: 10, 8: 11, 9: 12, 10: 13, 11: 14, 12: 15, 13: 16, 14: 17}

    def block(d):
        return nz(d) * 2 + c

    def give(m, *distances):
        for d in distances:
            from_partner[m, d] = same(bufs[m].at[block(d)], partner)

    def pieces(m, s, later=None):
        if s < 3 and later is None:
            return slice(None), slice(None)
        return (low, top) if later else (top, low)

    def issue(i):
        m, s = order[i][:2]
        ahead, behind = pieces(*order[i])
        from_down[i] = same(bufs[m].at[block(-s), ahead], up)
        from_up[i] = same(bufs[m].at[block(s), behind], down)
        if m == K and order[i][2:] != (1,):
            from_down[B, s] = same(gb.at[block(-s)], up)
            if s < 3:
                from_up[B, s] = same(gb.at[block(s)], down)

    def ring(*indices):
        for i in indices:
            m, s, *later = order[i]
            ahead, behind = pieces(*order[i])
            arrived(from_down[i], bufs[m].at[block(-s - 1), ahead])
            arrived(from_up[i], bufs[m].at[block(s + 1), behind])
            if m == K and later != [1]:
                arrived(from_down[B, s], gb.at[block(-s - 1)])
                if s < 3:
                    arrived(from_up[B, s], gb.at[block(s + 1)])
            if i in leave:
                issue(leave[i])
            if m == K and later != [1]:
                give(B, *((-s - 1, s + 1) if s < 3 else (4,)))
            if s == 3:
                give(m, 4)
            elif later != [0]:
                give(m, -s - 1, s + 1)

    def take(m, *distances):
        for d in distances:
            arrived(from_partner[m, d], bufs[m].at[nz(d) * 2 + (1 - c)])

    own_a, own_b = xg.at[y, x, top], xg.at[y, x, low]
    for i, needs in enumerate(((1,), (2,), (3, 4))):
        for j in needs:
            fetched[j].wait()
        issue(i)
        if i == 0:
            s = [same(own_a, xp), same(own_a, xd), same(own_b, yp), same(own_b, yd)]
    for copy in fetched[5:]:
        copy.wait()
    acc_q[...] = jnp.zeros_like(acc_q)
    acc_k[...] = jnp.zeros_like(acc_k)
    acc_v[...] = jnp.zeros_like(acc_v)
    logits[...] = jnp.zeros_like(logits)
    row = lax.broadcasted_iota(jnp.int32, (256, 128), 0)
    where = jnp.concatenate([pos_v[0:1, :], pos_v[1:2, :] + 128], axis=1)
    chosen = jnp.where(row == where, 1.0, 0.0).T.astype(BF16)

    arrived(s[0], xg.at[y, nx(-1), top])
    f0 = same(xg.at[y, nx(-1), a0], xp)
    arrived(s[1], xg.at[y, nx(1), top])
    f1 = same(xg.at[y, nx(1), a1], xd)
    arrived(s[2], xg.at[ny(-1), x, low])
    f2 = same(xg.at[ny(-1), x, b0], yp)
    arrived(s[3], xg.at[ny(1), x, low])
    f3 = same(xg.at[ny(1), x, b1], yd)
    arrived(f0, xg.at[y, nx(2), a0])
    arrived(f1, xg.at[y, nx(2), a1])
    rows_a = lambda yy, r: xg.at[yy, :, r]
    s0 = same(rows_a(y, top), yp)
    s1 = same(rows_a(y, top), yd)
    arrived(f2, xg.at[ny(2), x, b0])
    arrived(f3, xg.at[ny(2), x, b1])
    rows_b = lambda xx, r: xg.at[:, xx, r]
    s2 = same(rows_b(x, low), xp)
    s3 = same(rows_b(x, low), xd)
    ring(0, 1, 2)

    arrived(s0, rows_a(ny(-1), top))
    f0 = same(rows_a(ny(-1), a0), yp)
    arrived(s1, rows_a(ny(1), top))
    f1 = same(rows_a(ny(1), a1), yd)
    arrived(s2, rows_b(nx(-1), low))
    f2 = same(rows_b(nx(-1), b0), xp)
    arrived(s3, rows_b(nx(1), low))
    f3 = same(rows_b(nx(1), b1), xd)
    ring(3, 4)
    for m in (Q, O, V, K, B):
        give(m, 0)
    arrived(f0, rows_a(ny(2), a0))
    arrived(f1, rows_a(ny(2), a1))
    arrived(f2, rows_b(nx(2), b0))
    arrived(f3, rows_b(nx(2), b1))

    def squares(i, total):
        v = xg[i // 4, lax.rem(i, 4)].astype(F32)
        v = v * v
        return total + (v[:, 0:128] + v[:, 128:256])

    with jax.named_scope("squares"):
        total = lax.fori_loop(0, 16, squares, jnp.zeros((256, 128), F32))
        scale = lax.rsqrt(jnp.sum(total, axis=1, keepdims=True) * (1.0 / 4096) + EPS)
    ring(5)

    def normalise(i, carry):
        v = xg[i // 4, lax.rem(i, 4)].astype(F32)
        n = (v * scale).astype(BF16)
        xn[i] = n
        xm[i] = dot(chosen, n).astype(BF16)
        return carry

    with jax.named_scope("normalise"):
        lax.fori_loop(0, 16, normalise, 0)

    def project(m, *distances):
        take(m, *distances)
        if m == K:
            take(B, *distances)
        acc = {Q: acc_q, V: acc_v, K: acc_k}[m]
        left = xn if m == Q else xm
        for d in distances:
            i = nz(d) * 2
            acc[...] += dot(left[i], bufs[m][i]) + dot(left[i + 1], bufs[m][i + 1])
            if m == K:
                logits[...] += dot(left[i], gb[i], NT) + dot(left[i + 1], gb[i + 1], NT)

    ring(6)
    with jax.named_scope("project_q"):
        project(Q, 0, -1, 1, -2, 2)
    ring(7, 8, 9, 10)
    project(Q, -3, 3, 4)

    def wide_state(h):
        high, lo = split(state[h])
        return jnp.concatenate([high, lo, high], axis=1)

    def through(rows, wide):
        high, lo = split(rows)
        return dot(jnp.concatenate([high, high, lo], axis=1), wide, NT)

    cols = (slice(0, 128), slice(128, 256))
    seg_rows = (slice(0, 128), slice(128, 256))
    seg_mem = (slice(0, 64), slice(64, 128))

    def queries(seg, h):
        return acc_q[seg_rows[seg], cols[h]] * (128.0 ** -0.5)

    wides = [wide_state(h) for h in range(2)]
    for h in range(2):
        base[:, cols[h]] = through(queries(1, h), wides[h])
    readout = jnp.concatenate([through(queries(0, h), wides[h]) for h in range(2)], axis=1).astype(BF16)
    take(O, 0, -1, 1, -2, 2, -3, 3, 4)
    scatter = [
        Scatter(net, [r.at[seg] for r in sums], (nx, ny), (xp, xd, x2, yp, yd, y2)) for seg in range(2)
    ]
    with jax.named_scope("multiply0"):
        scatter[0].start(readout, go)
        scatter[0].push(False)
    project(K, 0, -1, 1)
    ring(11, 12)
    scatter[0].hand_on()
    ring(13)
    project(V, 0, -1, 1)
    ring(14)
    project(K, -2, 2)
    ring(15)
    project(V, -2, 2)
    ring(16)
    project(K, -3, 3)
    scatter[0].turn()
    project(V, -3, 3)
    project(K, 4)

    keys, betas, recalls, matches = [], [], [], []
    with jax.named_scope("prepare"):
        for h in range(2):
            k = acc_k[:, cols[h]]
            k = k * lax.rsqrt(jnp.sum(k * k, axis=1, keepdims=True) + 1e-06)
            keys.append(k)
            betas.append(jax.nn.sigmoid(logits[:, h:h + 1]))
            kh, kl = split(k[seg_mem[0]])
            match_high, match_low = split(through(queries(1, h), jnp.concatenate([kh, kl, kh], axis=1)))
            matches.append(jnp.concatenate([match_high, match_high, match_low], axis=1))
            recalls.append(through(k[seg_mem[0]], wide_state(h)))
    ring(17)
    project(V, 4)
    values = [acc_v[:, cols[h]] for h in range(2)]

    def change(seg, h, recalled):
        m = seg_mem[seg]
        return split(betas[h][m] * (values[h][m] - recalled))

    def update(seg, h, changed):
        ch, cl = changed
        kh, kl = split(keys[h][seg_mem[seg]])
        state[h] += dot(jnp.concatenate([ch, ch, cl], axis=0), jnp.concatenate([kh, kl, kh], axis=0), TN)

    with jax.named_scope("recur"):
        changes, readouts = [], []
        for h in range(2):
            ch, cl = change(0, h, recalls[h])
            changes.append((ch, cl))
            readouts.append(base[:, cols[h]] + dot(matches[h], jnp.concatenate([ch, cl, ch], axis=0)))
        readout = jnp.concatenate(readouts, axis=1).astype(BF16)
    with jax.named_scope("multiply1"):
        scatter[1].start(readout, go)

    for h in range(2):
        update(0, h, changes[h])
    scatter[1].push(True)
    for h in range(2):
        update(1, h, change(1, h, through(keys[h][seg_mem[1]], wide_state(h))))
    stored = []
    for h in range(2):
        copy = pltpu.make_async_copy(state.at[h], memory_ref.at[0, h], local.at[h])
        copy.start()
        stored.append(copy)

    def put_out(seg):
        for part in scatter[seg].last(xg.at[y, x], out_v, seg * 128):
            copy = pltpu.make_async_copy(out_v.at[part], out_ref.at[0, part], local.at[len(stored)])
            copy.start()
            stored.append(copy)

    scatter[1].hand_on()
    put_out(0)
    scatter[1].turn()
    with jax.named_scope("drain"):
        net.drain()
    put_out(1)
    with jax.named_scope("stored"):
        for copy in stored:
            copy.wait()


COPIES = 151


def finish(hidden_in, memory_in, hidden_out, memory_out, hidden, memory):
    def run(arrive, leave):
        moves = []
        for i in range(2):
            rows = slice(128 * i, 128 * i + 128)
            moves.append((hidden_in.at[0, rows], hidden.at[rows], hidden_out.at[0, rows]))
            moves.append((memory_in.at[0, i], memory.at[i], memory_out.at[0, i]))
        first = [pltpu.make_async_copy(src, via, arrive.at[i]) for i, (src, via, _) in enumerate(moves)]
        second = [pltpu.make_async_copy(via, dst, leave.at[i]) for i, (_, via, dst) in enumerate(moves)]
        for copy in first:
            copy.start()
        for before, after in zip(first, second):
            before.wait()
            after.start()
        for copy in second:
            copy.wait()

    pl.run_scoped(run, pltpu.SemaphoreType.DMA((4,)), pltpu.SemaphoreType.DMA((4,)))


def body(hidden_in, w_query, w_key, w_value, w_beta, w_out, mem_pos, memory_in):
    vmem = pltpu.VMEM
    scratch = [
        vmem((4, 4, 256, 256), BF16),
        vmem((16, 256, 256), BF16),
        vmem((16, 128, 256), BF16),
        vmem((16, 256, 256), BF16),
        vmem((16, 256, 256), BF16),
        vmem((16, 256, 256), BF16),
        vmem((16, 256, 256), BF16),
        vmem((16, 2, 256), BF16),
        vmem((2, 64), jnp.int32),
        vmem((2, 128, 128), F32),
        vmem((256, 256), BF16),
        vmem((256, 256), F32),
        vmem((128, 256), F32),
        vmem((128, 256), F32),
        vmem((128, 256), F32),
        vmem((128, 2), F32),
        vmem((2, 4, 4, 64, 256), BF16),
        vmem((2, 2, 4, 32, 256), BF16),
        vmem((2, 2, 4, 32, 256), BF16),
        vmem((2, 2, 4, 64, 256), BF16),
        vmem((2, 3, 64, 256), BF16),
        vmem((2, 64, 256), F32),
        vmem((2, 3, 64, 256), BF16),
        vmem((2, 4, 4, 64, 256), BF16),
        vmem((2, 2, 4, 32, 256), BF16),
        vmem((2, 2, 4, 32, 256), BF16),
        vmem((2, 2, 4, 64, 256), BF16),
        vmem((2, 3, 64, 256), BF16),
        vmem((2, 64, 256), F32),
        vmem((2, 3, 64, 256), BF16),
    ]
    results = pl.pallas_call(
        kernel,
        out_shape=(
            jax.ShapeDtypeStruct(hidden_in.shape, BF16),
            jax.ShapeDtypeStruct(memory_in.shape, F32),
        ),
        in_specs=[pl.BlockSpec(memory_space=pltpu.HBM)] * 8,
        out_specs=[pl.BlockSpec(memory_space=pltpu.HBM)] * 2,
        scratch_shapes=scratch,
        compiler_params=pltpu.CompilerParams(
            collective_id=0, has_side_effects=True
        ),
    )(hidden_in, w_query, w_key, w_value, w_beta.T, w_out, mem_pos, memory_in)
    return pl.pallas_call(
        finish,
        out_shape=[jax.ShapeDtypeStruct(r.shape, r.dtype) for r in results],
        in_specs=[pl.BlockSpec(memory_space=pltpu.HBM)] * 2,
        out_specs=[pl.BlockSpec(memory_space=pltpu.HBM)] * 2,
        scratch_shapes=[vmem((256, 256), BF16), vmem((2, 128, 128), F32)],
    )(*results)


def solution(mesh):
    split = Mesh(mesh.devices.reshape(4, 4, 8, 2), ("y", "x", "z", "c"))
    return jax.shard_map(
        body,
        mesh=split,
        in_specs=(
            P(BATCH, None, HEAD),
            P(BATCH, HEAD),
            P(BATCH, HEAD),
            P(BATCH, HEAD),
            P(BATCH, HEAD),
            P(HEAD, BATCH),
            P(BATCH, None, None),
            P(BATCH, HEAD, None, None),
        ),
        out_specs=(P(BATCH, None, HEAD), P(BATCH, HEAD, None, None)),
        check_vma=False,
    )
```
